512 devices in a mesh: phase: 8 (over y, core), wide: 64 (over x, z).
Axes of the slice: x: 4, y: 4, z: 16, core: 2. Of those that a mesh axis runs over, the one named last changes fastest.
Arguments:
- image: bfloat16 [16, 256, 16384], P(None, None, 'wide'), may hold values from -6 to 6
- conv_weight: bfloat16 [8, 256, 2304], P('phase'), may hold values from -0.09375 to 0.09375
- class_weight: bfloat16 [11, 256], replicated, may hold values from -0.375 to 0.375
- point_feats: float32 [16, 4, 16384], P('phase', None, 'wide'), may hold values from -6 to 6
- pixel_index: int32 [16, 16384], P('phase', 'wide'), may hold values from 0 to 16383
- pillar_index: int32 [16, 16384], P('phase', 'wide'), may hold values from 0 to 8191
- point_counts: int32 [16, 64], P('phase', 'wide'), may hold values from 64 to 256, as said below
- pillar_weight: float32 [64, 15], replicated, may hold values from -1.5 to 1.5
- bev_weight: bfloat16 [576, 384], replicated, may hold values from -0.25 to 0.25
- head_weight: bfloat16 [384, 20], replicated, may hold values from -0.3125 to 0.3125
Outputs:
- detections: float32 [16, 8192, 20], P('phase', 'wide')
- scores: float32 [16, 11, 16384], P('phase', None, 'wide')
The draws below stay inside these ranges and needn't reach their ends.
Inputs may be any that keep to these rules, and one draw needn't show every extreme that they name: `point_counts`: in every frame some index of wide has all 256 slots live; slots at or past the count are padding.
All inputs are finite; a program needn't handle non-finite values.
Results may differ from the reference program's by a relative error of at most 0.01.
Values may be sent and summed in bfloat16 or wider, within the bound.
A program may use at most 64 MiB of HBM per device.

```python
import jax
import jax.numpy as jnp
from jax import lax

C = 256
K = 11
PF = 4
PIL = 64
HEAD = 384
OUT = 20
IMG_W = 64
PTS_DEV = 256
BEV_W = 128
FRAMES = 16
PIX = 16384
PTS = 16384
BEV_H = 64
CELLS = 8192
N_PHASE = 8
N_WIDE = 64


def draw_point_counts(key, part):
    first_key = jax.random.fold_in(key, 11)
    second_key = jax.random.fold_in(key, 12)
    counts = jax.random.randint(first_key, (FRAMES, N_WIDE), PTS_DEV // 4, PTS_DEV + 1)
    fullest = jax.random.randint(second_key, (FRAMES, 1), 0, N_WIDE)
    positions = jnp.arange(N_WIDE, dtype=jnp.int32)[None, :]
    return jnp.where(positions == fullest, PTS_DEV, counts).astype(jnp.int32)


def set_ends(entries, stream_key, smallest, top_value):
    longest = entries.shape.index(max(entries.shape))
    spots = []
    for shift in (0, 1):
        where = [jax.random.randint(jax.random.fold_in(stream_key, axis), (), 0, length) for axis, length in enumerate(entries.shape)]
        where[longest] = (where[longest] + shift) % entries.shape[longest]
        spots.append(tuple(where))
    return entries.at[spots[0]].set(smallest).at[spots[1]].set(top_value)


def block_scale(rng, shape, shards, low, largest):
    loudness = 1.0
    for axis_at, parts in shards:
        heights = jax.random.uniform(jax.random.fold_in(jax.random.fold_in(rng, 6), axis_at), (parts,), jnp.float32, low / len(shards), largest / len(shards))
        loudness = loudness * jnp.repeat(jnp.exp(heights), shape[axis_at] // parts).reshape((-1,) + (1,) * (len(shape) - 1 - axis_at))
    return loudness


def normal_values(stream_key, dims, scale, limit, cuts=(), kind=jnp.bfloat16):
    array = scale * jax.random.normal(stream_key, dims, jnp.float32)
    if cuts:
        array = array * block_scale(stream_key, dims, cuts, -0.22, 0.18)
    return jnp.clip(array, -limit, limit).astype(kind)


def setup_inputs(seed: int = 0) -> dict:
    keys = jax.random.split(jax.random.key(seed), 11)
    return {
        "image": normal_values(keys[0], (FRAMES, C, PIX), 1.0, 6.0, ((2, 64),)),
        "conv_weight": normal_values(keys[1], (N_PHASE, C, 9 * C), (18 * C) ** -0.5, 0.09375, ((0, 8),)),
        "class_weight": normal_values(keys[2], (K, C), C ** -0.5, 0.375),
        "point_feats": normal_values(keys[3], (FRAMES, PF, PTS), 1.0, 6.0, ((0, 8), (2, 64)), jnp.float32),
        "pixel_index": set_ends(jax.random.randint(keys[4], (FRAMES, PTS), 0, PIX), jax.random.fold_in(keys[4], 1), 0, PIX - 1).astype(jnp.int32),
        "pillar_index": set_ends(jax.random.randint(keys[5], (FRAMES, PTS), 0, CELLS), jax.random.fold_in(keys[5], 1), 0, CELLS - 1).astype(jnp.int32),
        "point_counts": draw_point_counts(jax.random.fold_in(keys[10], 71), 0),
        "pillar_weight": normal_values(keys[7], (PIL, PF + K), (PF + K) ** -0.5, 1.5, (), jnp.float32),
        "bev_weight": normal_values(keys[8], (9 * PIL, HEAD), (9 * PIL) ** -0.5, 0.25),
        "head_weight": normal_values(keys[9], (HEAD, OUT), HEAD ** -0.5, 0.3125),
    }


def image_layer(activation, weight):
    frames, channels, height, breadth = activation.shape
    padded = jnp.pad(activation.astype(jnp.float32), ((0, 0), (0, 0), (1, 1), (1, 1)))
    running = jnp.zeros((frames, weight.shape[0], height, breadth), jnp.float32)
    for row_step in range(3):
        for col_step in range(3):
            tap_index = row_step * 3 + col_step
            window = padded[:, :, row_step:row_step + height, col_step:col_step + breadth]
            block = weight[:, tap_index * channels:(tap_index + 1) * channels].astype(jnp.float32)
            running = running + jnp.einsum("oc,fchw->fohw", block, window)
    return (activation.astype(jnp.float32) + jax.nn.relu(running)).astype(jnp.bfloat16)


def pool_frame(hidden_frame, index_frame):
    return jax.ops.segment_sum(hidden_frame.astype(jnp.float32).T, index_frame, num_segments=CELLS)


def reference(image, conv_weight, class_weight, point_feats, pixel_index, pillar_index, point_counts, pillar_weight, bev_weight, head_weight):
    frames = image.shape[0]
    height = image.shape[2] // IMG_W
    activation = image.reshape(frames, C, height, IMG_W)
    for layer_index in range(N_PHASE):
        activation = image_layer(activation, conv_weight[layer_index])
    flat = activation.reshape(frames, C, height * IMG_W)
    scores = jnp.einsum("kc,fcp->fkp", class_weight.astype(jnp.float32), flat.astype(jnp.float32))
    logits = scores.astype(jnp.bfloat16)
    spread_index = jnp.broadcast_to(pixel_index[:, None, :], (frames, K, PTS))
    painted = jnp.take_along_axis(logits.astype(jnp.float32), spread_index, axis=2)
    features = jnp.concatenate([point_feats, jax.nn.sigmoid(painted)], axis=1)
    hidden = jax.nn.relu(jnp.einsum("jd,fdp->fjp", pillar_weight, features, precision=lax.Precision.HIGHEST))
    slots = jnp.arange(PTS, dtype=jnp.int32)
    limits = point_counts[:, slots // PTS_DEV]
    is_live = (slots % PTS_DEV)[None, :] < limits
    hidden = jnp.where(is_live[:, None, :], hidden, 0.0).astype(jnp.bfloat16)
    pooled = jax.vmap(pool_frame)(hidden, pillar_index)
    grid = pooled.astype(jnp.bfloat16).reshape(frames, BEV_H, BEV_W, PIL).astype(jnp.float32)
    padded = jnp.pad(grid, ((0, 0), (1, 1), (1, 1), (0, 0)))
    running = jnp.zeros((frames, BEV_H, BEV_W, HEAD), jnp.float32)
    for row_step in range(3):
        for col_step in range(3):
            tap_index = row_step * 3 + col_step
            window = padded[:, row_step:row_step + BEV_H, col_step:col_step + BEV_W, :]
            block = bev_weight[tap_index * PIL:(tap_index + 1) * PIL].astype(jnp.float32)
            running = running + jnp.einsum("fhwj,jo->fhwo", window, block)
    feature = jax.nn.relu(running).astype(jnp.bfloat16).reshape(frames, CELLS, HEAD)
    detections = jnp.einsum("fcj,jo->fco", feature.astype(jnp.float32), head_weight.astype(jnp.float32))
    return (detections, scores)
```

```python
import functools

import jax
import jax.numpy as jnp
from jax import lax
from jax.experimental import pallas as pl
from jax.experimental.pallas import tpu as pltpu
from jax.sharding import PartitionSpec as P

C = 256
ROWS = 24
CHUNK = 8
M = CHUNK * 64
BUF = 1792
MESH = pl.DeviceIdType.MESH


def layers(act, weights, first_layer, last_layer, top_row):
    column = lax.broadcasted_iota(jnp.int32, (M, 1), 0) % 64
    has_left = column >= 1
    has_right = column < 63
    row_in_chunk = lax.broadcasted_iota(jnp.int32, (M, 1), 0) // 64

    def layer(number, carry):
        now, later = number % 2, (number + 1) % 2

        def chunk(step, inner):
            start = pl.multiple_of((number + 1) * 64 + step * M, 64)
            centre = act[now, pl.ds(start, M), :]
            lhs = jnp.concatenate(
                [act[now, pl.ds(start - 64, M), :], centre, act[now, pl.ds(start + 64, M), :]], axis=1
            )

            def part(tap):
                rhs = jnp.concatenate(
                    [weights[number, :, (3 * r + tap) * C : (3 * r + tap + 1) * C] for r in range(3)], axis=1
                )
                return lax.dot_general(
                    lhs, rhs, (((1,), (1,)), ((), ())), preferred_element_type=jnp.float32
                )

            total = part(1)
            total = total + jnp.where(has_left, pltpu.roll(part(0), 1, 0), 0.0)
            total = total + jnp.where(has_right, pltpu.roll(part(2), M - 1, 0), 0.0)
            row = top_row + start // 64 + row_in_chunk
            new = centre.astype(jnp.float32) + jnp.maximum(total, 0.0)
            new = jnp.where((row >= 0) & (row < 256), new, 0.0)
            act[later, pl.ds(start, M), :] = new.astype(jnp.bfloat16)
            return inner

        lax.fori_loop(0, (22 - 2 * number + CHUNK - 1) // CHUNK, chunk, 0)
        return carry

    lax.fori_loop(first_layer, last_layer, layer, 0)


def image_kernel(
    img, w_own, cwq, pts, sc, table, points, weights, act,
    own_sem, send_sem, h_sem, y1_sem, y2_sem, x1_sem, x2_sem, d_sem, tz_sem, tx_sem, pz_sem, px_sem, s_sem, ag_send,
):
    p = lax.axis_index("phase")
    w = lax.axis_index("wide")
    y, c = p // 2, p % 2
    x, z = w // 16, w % 16
    k, t = w // 2, w % 2
    top_row = 8 * k - 8

    def at(phase, wide):
        return {"phase": phase, "wide": wide}

    def y_dev(step):
        return at(2 * ((y + step + 4) % 4) + c, w)

    def x_dev(step):
        return at(p, 16 * ((x + step + 4) % 4) + z)

    def z_dev(step):
        return at(p, 16 * x + (z + step) % 16)

    partner = at(2 * y + 1 - c, w)
    sibling = at(p, 2 * k + 1 - t)
    halo_peers = [(d, f) for d in (-1, 1) for f in (0, 1)]

    own_copy = pltpu.make_async_copy(w_own.at[0], weights.at[p], own_sem)
    own_copy.start()
    barrier = pltpu.get_barrier_semaphore()
    peers = [y_dev(1), y_dev(-1), partner, sibling]
    peers += [x_dev(e) for e in (1, 2, 3)] + [z_dev(d) for d in range(1, 16)]
    peers += [at(p, (2 * (k + d) + f + 64) % 64) for d, f in halo_peers]
    for peer in peers:
        pl.semaphore_signal(barrier, inc=1, device_id=peer, device_id_type=MESH)
    pl.semaphore_wait(barrier, len(peers))

    sends = []

    def send(src, dst, recv, device):
        number = len(sends)
        copy = pltpu.make_async_remote_copy(
            src_ref=src, dst_ref=dst, send_sem=send_sem.at[number], recv_sem=recv,
            device_id=device, device_id_type=MESH,
        )
        copy.start()
        sends.append(copy)

    def arrived(ref, recv):
        pltpu.make_async_remote_copy(
            src_ref=ref, dst_ref=ref, send_sem=send_sem.at[0], recv_sem=recv,
            device_id=partner, device_id_type=MESH,
        ).wait_recv()

    def block(j):
        return act.at[0, pl.ds(pl.multiple_of(j * 256, 256), 256), :]

    send(img.at[1 - t], block(2 + t), h_sem.at[2 + t], sibling)
    for d, f in halo_peers:
        send(img.at[f], block(2 - 2 * d + t), h_sem.at[2 - 2 * d + t], at(p, (2 * (k + d) + f + 64) % 64))

    def q_cols(layer, owner, first=0, tiles=3):
        return weights.at[layer, :, pl.ds(pl.multiple_of(768 + 384 * owner + 128 * first, 128), 128 * tiles)]

    def a_cols(layer, first=0, tiles=6):
        return weights.at[layer, :, pl.ds(128 * first, 128 * tiles)]

    def layer_of(step):
        return 2 * ((y + step + 8) % 4) + c

    sign = 1 - 2 * c
    own_copy.wait()
    for d in range(2):
        step = sign * (1 - 2 * d)
        send(q_cols(p, x), q_cols(p, x), y1_sem.at[d, 0], y_dev(step))
    for d in range(2):
        step = sign * (1 - 2 * d)
        send(a_cols(p), a_cols(p), y1_sem.at[d, 1], y_dev(step))
    send(weights.at[p], weights.at[p], d_sem.at[3], partner)

    q_parts = ((0, 2), (2, 1))
    a_parts = ((0, 3), (3, 3))
    near = [layer_of(-sign), layer_of(sign)]
    far = layer_of(2)

    def x_first(layer, j):
        for d in range(2):
            send(q_cols(layer, x), q_cols(layer, x), x1_sem.at[d, j], x_dev(sign * (1 - 2 * d)))

    def x_second(layer, j):
        for d in range(2):
            step = sign * (1 - 2 * d)
            source = (x - step + 4) % 4
            arrived(q_cols(layer, source), x1_sem.at[d, j])
            part = q_cols(layer, source, *q_parts[d])
            send(part, part, x2_sem.at[d, j], x_dev(step))

    def x_done(layer, j):
        for d in range(2):
            arrived(q_cols(layer, (x + 2) % 4, *q_parts[d]), x2_sem.at[d, j])

    for d in range(2):
        step = sign * (1 - 2 * d)
        arrived(q_cols(near[d], x), y1_sem.at[d, 0])
        part = q_cols(near[d], x, *q_parts[d])
        send(part, part, y2_sem.at[d, 0], y_dev(step))
    for d in range(2):
        x_first(near[d], d)
    for d in range(2):
        step = sign * (1 - 2 * d)
        arrived(a_cols(near[d]), y1_sem.at[d, 1])
        part = a_cols(near[d], *a_parts[d])
        send(part, part, y2_sem.at[d, 1], y_dev(step))
    for d in range(2):
        arrived(q_cols(far, x, *q_parts[d]), y2_sem.at[d, 0])
    x_first(far, 2)
    for d in range(2):
        x_second(near[d], d)
    for d in range(2):
        x_done(near[d], d)
        send(weights.at[near[d]], weights.at[near[d]], d_sem.at[d], partner)
    x_second(far, 2)
    for d in range(2):
        arrived(a_cols(far, *a_parts[d]), y2_sem.at[d, 1])
    x_done(far, 2)
    send(weights.at[far], weights.at[far], d_sem.at[2], partner)

    order = (8, 7, 9, 6, 10, 5, 11, 4, 12, 3, 13, 2, 14, 1, 15)

    def spread_z(ref, sem, number):
        own = ref.at[w]
        for d in order:
            pltpu.make_async_remote_copy(
                src_ref=own, dst_ref=own, send_sem=ag_send.at[number], recv_sem=sem.at[d],
                device_id=z_dev(d), device_id_type=MESH,
            ).start()

    def forward(ref, sem, source, number):
        for e in (1, 2, 3):
            pltpu.make_async_remote_copy(
                src_ref=ref.at[source], dst_ref=ref.at[source], send_sem=ag_send.at[number], recv_sem=sem.at[e],
                device_id=x_dev(e), device_id_type=MESH,
            ).start()

    def spread_x(ref, z_sem, x_sem, number):
        forward(ref, x_sem, w, number)
        for d in reversed(order):
            source = 16 * x + (z - d + 16) % 16
            arrived(ref.at[source], z_sem.at[d])
            forward(ref, x_sem, source, number)

    def spread_end(ref, x_sem, number):
        for e in (1, 2, 3):
            arrived(ref.at[pl.ds(16 * ((x - e + 4) % 4), 16)], x_sem.at[e])
        pltpu.make_async_remote_copy(
            src_ref=ref.at[pl.ds(0, 63)], dst_ref=ref.at[pl.ds(0, 63)], send_sem=ag_send.at[number],
            recv_sem=own_sem, device_id=partner, device_id_type=MESH,
        ).wait_send()

    points[w] = pts[...]
    spread_z(points, pz_sem, 0)

    act[0, pl.ds(pl.multiple_of((2 + t) * 256, 256), 256), :] = img[t]
    for j in (0, 1, 4, 5):
        arrived(block(j), h_sem.at[j])
    arrived(block(3 - t), h_sem.at[3 - t])

    @pl.when(k == 0)
    def _():
        act[0, pl.ds(0, 512), :] = jnp.zeros((512, C), jnp.bfloat16)

    @pl.when(k == 31)
    def _():
        act[0, pl.ds(1024, 512), :] = jnp.zeros((512, C), jnp.bfloat16)

    other = 1 - c
    their_sign = 1 - 2 * other
    theirs = [2 * ((y - their_sign + 4) % 4) + other, 2 * ((y + their_sign + 4) % 4) + other,
              2 * ((y + 2) % 4) + other, 2 * y + other]
    for j in (3, 0, 1, 2):
        arrived(weights.at[theirs[j]], d_sem.at[j])

    layers(act, weights, 0, 4, top_row)
    spread_x(points, pz_sem, px_sem, 0)
    layers(act, weights, 4, 8, top_row)

    total = None
    for q in range(4):
        part = lax.dot_general(
            cwq[q], act[0, pl.ds(512 + 128 * q, 128), :], (((1,), (1,)), ((), ())),
            preferred_element_type=jnp.float32,
        )
        total = part if total is None else total + part
    table[w] = total.astype(jnp.bfloat16)
    sc[t] = total
    spread_z(table, tz_sem, 1)
    send(sc.at[t], sc.at[t], s_sem, sibling)
    spread_x(table, tz_sem, tx_sem, 1)
    spread_end(points, px_sem, 0)
    spread_end(table, tx_sem, 1)
    arrived(sc.at[1 - t], s_sem)
    for copy in sends:
        copy.wait_send()


N_SENDS = 48


def image_part(img, conv_weight, cwq, pts):
    vmem = pl.BlockSpec(memory_space=pltpu.VMEM)
    dma = pltpu.SemaphoreType.DMA
    return pl.pallas_call(
        image_kernel,
        name="image_part",
        out_shape=(
            jax.ShapeDtypeStruct((2, 48, 128), jnp.float32),
            jax.ShapeDtypeStruct((64, 48, 128), jnp.bfloat16),
            jax.ShapeDtypeStruct((64, 32, 128), jnp.float32),
        ),
        in_specs=[vmem, pl.BlockSpec(memory_space=pl.ANY), vmem, vmem],
        out_specs=(vmem, vmem, vmem),
        scratch_shapes=[
            pltpu.VMEM((8, C, 9 * C), jnp.bfloat16),
            pltpu.VMEM((2, BUF, C), jnp.bfloat16),
            dma, dma((N_SENDS,)), dma((6,)), dma((2, 2)), dma((2, 2)), dma((2, 3)), dma((2, 3)), dma((4,)),
            dma((16,)), dma((4,)), dma((16,)), dma((4,)), dma, dma((2,)),
        ],
        compiler_params=pltpu.CompilerParams(
            collective_id=0, has_side_effects=True, vmem_limit_bytes=40 * 2**20
        ),
        cost_estimate=pl.CostEstimate(flops=10**10, bytes_accessed=10**7, transcendentals=0),
    )(img, conv_weight, cwq, pts)


SLOTS = 128
GROUP = 16
LANES = 256


def point_kernel(points, table, wk, bev, head, out, place, packed, pooled):
    w = lax.axis_index("wide")
    first_cell = ((w - 1) * 128).astype(jnp.float32)
    one, zero = jnp.float32(1.0), jnp.float32(0.0)

    def iota(shape, dim):
        return lax.broadcasted_iota(jnp.int32, shape, dim).astype(jnp.float32)

    def where_bf16(mask):
        return jnp.where(mask, one, zero).astype(jnp.bfloat16)

    def split(value):
        high = value.astype(jnp.bfloat16)
        return high, (value - high.astype(jnp.float32)).astype(jnp.bfloat16)

    row_i = lax.broadcasted_iota(jnp.int32, (128, 128), 0)
    col_i = lax.broadcasted_iota(jnp.int32, (128, 128), 1)
    up_to = where_bf16(row_i <= col_i)
    row_j = lax.broadcasted_iota(jnp.int32, (64, 64), 0)
    col_j = lax.broadcasted_iota(jnp.int32, (64, 64), 1)
    before = where_bf16((row_j // GROUP == col_j // GROUP) & (col_j < row_j))
    all_ones = jnp.ones((128, 128), jnp.bfloat16)
    slot_row = iota((SLOTS, 128), 0)
    low_row = iota((128, LANES), 0)
    quarter_row = lax.broadcasted_iota(jnp.int32, (48, LANES), 0) // 11
    quarter_row = quarter_row.astype(jnp.float32)
    class_i = lax.broadcasted_iota(jnp.int32, (16, 48), 0)
    class_j = lax.broadcasted_iota(jnp.int32, (16, 48), 1)
    to_class = where_bf16((class_j % 11 == class_i) & (class_j < 44))
    wk_high, wk_low = split(wk[...])
    wk_both = jnp.concatenate([wk_high, wk_low], axis=0)
    column = lax.broadcasted_iota(jnp.int32, (128, 1), 0)

    def frame(f, carry):
        most = zero
        for h in range(2):
            cell = points[pl.ds((2 * f + h) * 8 + 5, 64, stride=32), :] - first_cell
            mine = (cell >= 0.0) & (cell < 384.0)
            mine_16 = where_bf16(mine)
            inside = jnp.dot(mine_16, up_to, preferred_element_type=jnp.float32)
            row_sum = jnp.dot(mine_16, all_ones, preferred_element_type=jnp.float32)
            ahead = jnp.dot(before, row_sum.astype(jnp.bfloat16), preferred_element_type=jnp.float32)
            place[h] = jnp.where(mine, inside - 1.0 + ahead, -1.0)
            most = jnp.maximum(most, jnp.max(row_sum + ahead))
        passes = (most.astype(jnp.int32) + SLOTS - 1) // SLOTS
        pooled[...] = jnp.zeros_like(pooled)

        def one_pass(number, inner):
            slot = slot_row + (number * SLOTS).astype(jnp.float32)

            def group(g, state):
                h, first = g // 4, pl.multiple_of(g % 4 * GROUP, GROUP)
                places = place[h, pl.ds(first, GROUP), :]
                data, picks = [], []
                for i in range(GROUP):
                    rows = points[pl.ds(pl.multiple_of((first + i) * 32 + (2 * f + h) * 8, 8), 8), :]
                    high, low = split(rows)
                    data.append(jnp.concatenate([high.astype(jnp.float32), low.astype(jnp.float32)], axis=0))
                    picks.append(where_bf16(slot == places[i : i + 1, :]))
                chosen = lax.dot_general(
                    jnp.concatenate(data, axis=1).astype(jnp.bfloat16), jnp.concatenate(picks, axis=1),
                    (((1,), (1,)), ((), ())), preferred_element_type=jnp.float32,
                )
                packed[g] = chosen
                return state

            lax.fori_loop(0, 8, group, 0)

            def lanes(s, state):
                chosen = jnp.concatenate([packed[2 * s], packed[2 * s + 1]], axis=1)
                value = chosen[:8] + chosen[8:]
                pixel, cell, used = value[4:5], value[5:6] - first_cell, value[6:7]
                block = jnp.floor(pixel * (1.0 / 128.0))
                low = pixel - 128.0 * block
                pair = jnp.floor(block * 0.25)
                quarter = block - 4.0 * pair
                of_frame = jnp.concatenate([table[2 * i + f] for i in range(32)], axis=0)
                read = jnp.dot(of_frame, where_bf16(low_row == low), preferred_element_type=jnp.float32)
                total = jnp.zeros((48, LANES), jnp.float32)
                for i in range(32):
                    total = total + jnp.where(pair == float(i), read[48 * i : 48 * i + 48], 0.0)
                total = jnp.where(quarter_row == quarter, total, 0.0)
                painted = jnp.dot(to_class, total.astype(jnp.bfloat16), preferred_element_type=jnp.float32)
                gate = jax.nn.sigmoid(painted)
                gate_high, gate_low = split(gate)
                features = jnp.concatenate([chosen.astype(jnp.bfloat16), gate_high, gate_low], axis=0)
                both = jnp.dot(wk_both, features, preferred_element_type=jnp.float32)
                hidden = jnp.maximum(both[:64] + both[64:], 0.0)
                row = jnp.floor(cell * (1.0 / 128.0))
                col = cell - 128.0 * row
                row = jnp.where(used > 0.5, row, -1.0)
                by_row = jnp.concatenate(
                    [jnp.where(row == float(r), hidden, 0.0) for r in range(3)], axis=0
                ).astype(jnp.bfloat16)
                pooled[...] += lax.dot_general(
                    where_bf16(low_row == col), by_row, (((1,), (1,)), ((), ())),
                    preferred_element_type=jnp.float32,
                )
                return state

            lax.fori_loop(0, 8 * SLOTS // LANES, lanes, 0)
            return inner

        lax.fori_loop(0, passes, one_pass, 0)
        grid = pooled[...]
        total = None
        for d in range(3):
            if d == 0:
                moved = jnp.where(column >= 1, pltpu.roll(grid, 1, 0), 0.0)
            elif d == 2:
                moved = jnp.where(column < 127, pltpu.roll(grid, 127, 0), 0.0)
            else:
                moved = grid
            weight = jnp.concatenate([bev[(3 * r + d) * 64 : (3 * r + d + 1) * 64, :] for r in range(3)], axis=0)
            part = jnp.dot(moved.astype(jnp.bfloat16), weight, preferred_element_type=jnp.float32)
            total = part if total is None else total + part
        feature = jnp.maximum(total, 0.0).astype(jnp.bfloat16)
        out[f] = jnp.dot(feature, head[...], preferred_element_type=jnp.float32)
        return carry

    lax.fori_loop(0, 2, frame, 0)


def point_part(points, table, wk, bev, head):
    vmem = pl.BlockSpec(memory_space=pltpu.VMEM)
    return pl.pallas_call(
        point_kernel,
        name="point_part",
        out_shape=jax.ShapeDtypeStruct((2, 128, 20), jnp.float32),
        in_specs=[vmem] * 5,
        out_specs=vmem,
        scratch_shapes=[
            pltpu.VMEM((2, 64, 128), jnp.float32),
            pltpu.VMEM((8, 16, SLOTS), jnp.float32),
            pltpu.VMEM((128, 192), jnp.float32),
        ],
        compiler_params=pltpu.CompilerParams(vmem_limit_bytes=40 * 2**20),
        cost_estimate=pl.CostEstimate(flops=10**9, bytes_accessed=3 * 10**6, transcendentals=10**5),
    )(points, table, wk, bev, head)


def local(
    image,
    conv_weight,
    class_weight,
    point_feats,
    pixel_index,
    pillar_index,
    point_counts,
    pillar_weight,
    bev_weight,
    head_weight,
):
    p = lax.axis_index("phase")
    t = lax.axis_index("wide") % 2
    img = jnp.swapaxes(lax.dynamic_slice_in_dim(image, 2 * p, 2, 0), 1, 2)
    live = jnp.arange(256, dtype=jnp.int32)[None, :] < point_counts
    cell = jnp.where(live, pillar_index, -1024)
    used = jnp.ones((2, 1, 256), jnp.float32)
    rows = [point_feats, pixel_index[:, None].astype(jnp.float32), cell[:, None].astype(jnp.float32), used, used]
    pts = jnp.concatenate(rows, axis=1).reshape(2, 8, 2, 128).transpose(0, 2, 1, 3).reshape(32, 128)
    cwq = jnp.stack([jnp.pad(class_weight, ((11 * q, 37 - 11 * q), (0, 0))) for q in range(4)])
    sc, table, points = image_part(img, conv_weight, cwq, pts)
    own = lax.dynamic_slice_in_dim(sc[:, :44].reshape(2, 4, 11, 128), 2 * t, 2, 1)
    scores = own.transpose(0, 2, 1, 3).reshape(2, 11, 256)
    raw, gates = pillar_weight[:, :4], jnp.pad(pillar_weight[:, 4:], ((0, 0), (0, 5)))
    raw = jnp.pad(raw, ((0, 0), (0, 4)))
    wk = jnp.concatenate([raw, raw, gates, gates], axis=1)
    detections = point_part(points.reshape(64 * 32, 128), table, wk, bev_weight, head_weight)
    return (detections, scores)


def solution(mesh):
    placed = (
        P(None, None, "wide"),
        P("phase", None, None),
        P(),
        P("phase", None, "wide"),
        P("phase", "wide"),
        P("phase", "wide"),
        P("phase", "wide"),
        P(),
        P(),
        P(),
    )
    return jax.shard_map(
        local,
        mesh=mesh,
        in_specs=placed,
        out_specs=(P("phase", "wide", None), P("phase", None, "wide")),
        check_vma=False,
    )
```

```python
import functools

import jax
import jax.numpy as jnp
from jax import lax
from jax.experimental import pallas as pl
from jax.experimental.pallas import tpu as pltpu
from jax.sharding import PartitionSpec as P

C = 256
ROWS = 24
MOST_ROWS = 12
MESH = pl.DeviceIdType.MESH
NEAR = (4, -4, 3, -3, 2, -2, 1, -1)
EARLY = (0, 4, -4, 1, -1, 2, -2, 3, -3)
LATE = (5, -5, 6, -6, 7, -7, 8)


def layers(act, weights, numbers, top_row):
    for number in numbers:
        now, later = number % 2, (number + 1) % 2
        rows = 22 - 2 * number
        half = rows if rows <= MOST_ROWS else (rows + 1) // 2
        for first in range(0, rows, half):
            count = min(half, rows - first) * 64
            start = (number + 1 + first) * 64
            column = lax.broadcasted_iota(jnp.int32, (count, 1), 0) % 64
            row = lax.broadcasted_iota(jnp.int32, (count, 1), 0) // 64 + (top_row + number + 1 + first)
            lhs = jnp.concatenate([act[now, pl.ds(start + 64 * r, count), :] for r in (-1, 0, 1)], axis=1)

            def part(tap):
                rhs = jnp.concatenate(
                    [weights[number, :, (3 * r + tap) * C : (3 * r + tap + 1) * C] for r in range(3)], axis=1
                )
                return lax.dot_general(lhs, rhs, (((1,), (1,)), ((), ())), preferred_element_type=jnp.float32)

            total = part(1)
            total = total + jnp.where(column >= 1, pltpu.roll(part(0), 1, 0), 0.0)
            total = total + jnp.where(column < 63, pltpu.roll(part(2), count - 1, 0), 0.0)
            new = act[now, pl.ds(start, count), :].astype(jnp.float32) + jnp.maximum(total, 0.0)
            new = jnp.where((row >= 0) & (row < 256), new, 0.0)
            act[later, pl.ds(start, count), :] = new.astype(jnp.bfloat16)


def image_kernel(
    image, w_own, class_weight, feats, pixel, pillar, counts, sc, table, points, weights, act, raw, img,
    own_sem, raw_sem, send_sem, h_sem, y1_sem, y2_sem, x1_sem, x2_sem, d_sem, tz_sem, tx_sem, tf_sem,
    pz_sem, px_sem, pf_sem, s_sem, ag_send,
):
    p = lax.axis_index("phase")
    w = lax.axis_index("wide")
    y, c = p // 2, p % 2
    x, z = w // 16, w % 16
    k, t = w // 2, w % 2
    top_row = 8 * k - 8

    def at(phase, wide):
        return {"phase": phase, "wide": wide}

    def y_dev(step):
        return at(2 * ((y + step + 4) % 4) + c, w)

    def x_dev(step):
        return at(p, 16 * ((x + step + 4) % 4) + z)

    def z_dev(step):
        return at(p, 16 * x + (z + step + 16) % 16)

    partner = at(2 * y + 1 - c, w)
    sibling = at(p, 2 * k + 1 - t)
    halo_peers = [(d, f) for d in (-1, 1) for f in (0, 1)]

    raw_copy = pltpu.make_async_copy(image.at[pl.ds(2 * p, 2)], raw, raw_sem)
    raw_copy.start()
    own_copy = pltpu.make_async_copy(w_own.at[0], weights.at[p], own_sem)
    own_copy.start()
    barrier = pltpu.get_barrier_semaphore()
    peers = [y_dev(1), y_dev(-1), partner, sibling]
    peers += [x_dev(1), x_dev(-1)] + [z_dev(d) for d in NEAR]
    peers += [at(p, (2 * (k + d) + f + 64) % 64) for d, f in halo_peers]
    for peer in peers:
        pl.semaphore_signal(barrier, inc=1, device_id=peer, device_id_type=MESH)
    lane = lax.broadcasted_iota(jnp.int32, (1, 256), 1)
    for f in range(2):
        cell = jnp.where(lane < counts[f : f + 1, :], pillar[f : f + 1, :], -1024).astype(jnp.float32)
        where = pixel[f : f + 1, :].astype(jnp.float32)
        for h in range(2):
            first = (2 * f + h) * 8
            points[w, first : first + 4, :] = feats[f, :, 128 * h : 128 * h + 128]
            points[w, first + 4 : first + 5, :] = where[:, 128 * h : 128 * h + 128]
            points[w, first + 5 : first + 6, :] = cell[:, 128 * h : 128 * h + 128]
            points[w, first + 6 : first + 8, :] = jnp.ones((2, 128), jnp.float32)
    raw_copy.wait()
    for f in range(2):
        img[f] = jnp.swapaxes(raw[f], 0, 1)
    pl.semaphore_wait(barrier, len(peers))

    sends = []

    def send(src, dst, recv, device):
        number = len(sends)
        copy = pltpu.make_async_remote_copy(
            src_ref=src, dst_ref=dst, send_sem=send_sem.at[number], recv_sem=recv,
            device_id=device, device_id_type=MESH,
        )
        copy.start()
        sends.append(copy)

    def arrived(ref, recv):
        pltpu.make_async_remote_copy(
            src_ref=ref, dst_ref=ref, send_sem=send_sem.at[0], recv_sem=recv,
            device_id=partner, device_id_type=MESH,
        ).wait_recv()

    def block(j):
        return act.at[0, pl.ds(pl.multiple_of(j * 256, 256), 256), :]

    send(img.at[1 - t], block(2 + t), h_sem.at[2 + t], sibling)
    for d, f in halo_peers:
        send(img.at[f], block(2 - 2 * d + t), h_sem.at[2 - 2 * d + t], at(p, (2 * (k + d) + f + 64) % 64))

    def post(src, sem, number, device):
        pltpu.make_async_remote_copy(
            src_ref=src, dst_ref=src, send_sem=ag_send.at[number], recv_sem=sem,
            device_id=device, device_id_type=MESH,
        ).start()

    class Spread:
        def __init__(self, ref, z_sem, x_sem, f_sem, number):
            self.ref, self.z_sem, self.x_sem, self.f_sem, self.number = ref, z_sem, x_sem, f_sem, number

        def block(self, d, column=0):
            return self.ref.at[16 * ((x + column + 4) % 4) + (z - d + 16) % 16]

        def z_first(self):
            for d in NEAR:
                post(self.block(0), self.z_sem.at[d % 16], self.number, z_dev(d))

        def z_wait(self, d):
            arrived(self.block(d), self.z_sem.at[d % 16])

        def z_second(self):
            for d in (4, -4):
                self.z_wait(d)
                for e in (4, 3, 2, 1) if d > 0 else (-3, -2, -1):
                    post(self.block(d), self.z_sem.at[(d + e) % 16], self.number, z_dev(e))

        def x_first(self, d):
            for side in range(2):
                post(self.block(d), self.x_sem.at[side, d % 16], self.number, x_dev(1 - 2 * side))

        def x_second(self, d):
            for side in range(2):
                step = 1 - 2 * side
                arrived(self.block(d, -step), self.x_sem.at[side, d % 16])
                if d % 2 == side:
                    post(self.block(d, -step), self.f_sem, self.number, x_dev(step))

        def end(self):
            arrived(self.ref.at[pl.ds(16 * ((x + 2) % 4), 16)], self.f_sem)
            pltpu.make_async_remote_copy(
                src_ref=self.ref.at[pl.ds(0, 63)], dst_ref=self.ref.at[pl.ds(0, 63)],
                send_sem=ag_send.at[self.number], recv_sem=own_sem, device_id=partner, device_id_type=MESH,
            ).wait_send()

    spread_points = Spread(points, pz_sem, px_sem, pf_sem, 0)
    spread_table = Spread(table, tz_sem, tx_sem, tf_sem, 1)

    def q_cols(layer, owner, first=0, tiles=3):
        return weights.at[layer, :, pl.ds(pl.multiple_of(768 + 384 * owner + 128 * first, 128), 128 * tiles)]

    def a_cols(layer, first=0, tiles=6):
        return weights.at[layer, :, pl.ds(128 * first, 128 * tiles)]

    def layer_of(step):
        return 2 * ((y + step + 8) % 4) + c

    sign = 1 - 2 * c
    own_copy.wait()
    for d in range(2):
        step = sign * (1 - 2 * d)
        send(q_cols(p, x), q_cols(p, x), y1_sem.at[d, 0], y_dev(step))
    for d in range(2):
        step = sign * (1 - 2 * d)
        send(a_cols(p), a_cols(p), y1_sem.at[d, 1], y_dev(step))
    send(weights.at[p], weights.at[p], d_sem.at[3], partner)
    spread_points.z_first()

    q_parts = ((0, 2), (2, 1))
    a_parts = ((0, 3), (3, 3))
    near = [layer_of(-sign), layer_of(sign)]
    far = layer_of(2)

    def x_first(layer, j):
        for d in range(2):
            send(q_cols(layer, x), q_cols(layer, x), x1_sem.at[d, j], x_dev(sign * (1 - 2 * d)))

    def x_second(layer, j):
        for d in range(2):
            step = sign * (1 - 2 * d)
            source = (x - step + 4) % 4
            arrived(q_cols(layer, source), x1_sem.at[d, j])
            part = q_cols(layer, source, *q_parts[d])
            send(part, part, x2_sem.at[d, j], x_dev(step))

    def x_done(layer, j):
        for d in range(2):
            arrived(q_cols(layer, (x + 2) % 4, *q_parts[d]), x2_sem.at[d, j])

    for d in range(2):
        step = sign * (1 - 2 * d)
        arrived(q_cols(near[d], x), y1_sem.at[d, 0])
        part = q_cols(near[d], x, *q_parts[d])
        send(part, part, y2_sem.at[d, 0], y_dev(step))
    for d in range(2):
        x_first(near[d], d)
    for d in range(2):
        step = sign * (1 - 2 * d)
        arrived(a_cols(near[d]), y1_sem.at[d, 1])
        part = a_cols(near[d], *a_parts[d])
        send(part, part, y2_sem.at[d, 1], y_dev(step))
    for d in range(2):
        arrived(q_cols(far, x, *q_parts[d]), y2_sem.at[d, 0])
    x_first(far, 2)
    for d in range(2):
        x_second(near[d], d)
    for d in range(2):
        x_done(near[d], d)
        send(weights.at[near[d]], weights.at[near[d]], d_sem.at[d], partner)
    x_second(far, 2)
    spread_points.z_second()
    for d in range(2):
        arrived(a_cols(far, *a_parts[d]), y2_sem.at[d, 1])
    x_done(far, 2)
    send(weights.at[far], weights.at[far], d_sem.at[2], partner)

    act[0, pl.ds(pl.multiple_of((2 + t) * 256, 256), 256), :] = img[t]
    for j in (0, 1, 4, 5):
        arrived(block(j), h_sem.at[j])
    arrived(block(3 - t), h_sem.at[3 - t])

    @pl.when(k == 0)
    def _():
        act[0, pl.ds(0, 512), :] = jnp.zeros((512, C), jnp.bfloat16)

    @pl.when(k == 31)
    def _():
        act[0, pl.ds(1024, 512), :] = jnp.zeros((512, C), jnp.bfloat16)

    other = 1 - c
    their_sign = 1 - 2 * other
    theirs = [2 * ((y - their_sign + 4) % 4) + other, 2 * ((y + their_sign + 4) % 4) + other,
              2 * ((y + 2) % 4) + other, 2 * y + other]
    for j in (3, 0, 1, 2):
        arrived(weights.at[theirs[j]], d_sem.at[j])

    layers(act, weights, (0, 1), top_row)
    for d in EARLY + LATE:
        if d not in (0, 4, -4):
            spread_points.z_wait(d)
        spread_points.x_first(d)
    layers(act, weights, (2, 3, 4, 5), top_row)
    for d in EARLY + LATE:
        spread_points.x_second(d)
    layers(act, weights, (6, 7), top_row)

    row_i = lax.broadcasted_iota(jnp.int32, (48, 11), 0)
    row_j = lax.broadcasted_iota(jnp.int32, (48, 11), 1)
    placed = []
    for q in range(4):
        here = jnp.where(row_i == row_j + 11 * q, 1.0, 0.0).astype(jnp.bfloat16)
        placed.append(
            jnp.dot(here, class_weight[...], preferred_element_type=jnp.float32).astype(jnp.bfloat16)
        )
    total = None
    for q in range(4):
        part = lax.dot_general(
            placed[q], act[0, pl.ds(512 + 128 * q, 128), :], (((1,), (1,)), ((), ())),
            preferred_element_type=jnp.float32,
        )
        total = part if total is None else total + part
    table[w] = total.astype(jnp.bfloat16)
    sc[t] = total
    spread_table.z_first()
    spread_table.x_first(0)
    send(sc.at[t], sc.at[t], s_sem, sibling)
    spread_table.z_second()
    spread_table.x_first(4)
    spread_table.x_first(-4)
    for d in (1, -1, 2, -2, 3, -3):
        spread_table.z_wait(d)
        spread_table.x_first(d)
    for d in EARLY:
        spread_table.x_second(d)
    for d in LATE:
        spread_table.z_wait(d)
        spread_table.x_first(d)
    for d in LATE:
        spread_table.x_second(d)
    spread_points.end()
    spread_table.end()
    arrived(sc.at[1 - t], s_sem)
    for copy in sends:
        copy.wait_send()


N_SENDS = 48


def image_part(image, conv_weight, class_weight, feats, pixel, pillar, counts):
    vmem = pl.BlockSpec(memory_space=pltpu.VMEM)
    hbm = pl.BlockSpec(memory_space=pltpu.HBM)
    dma = pltpu.SemaphoreType.DMA
    return pl.pallas_call(
        image_kernel,
        name="image_part",
        out_shape=(
            jax.ShapeDtypeStruct((2, 48, 128), jnp.float32),
            jax.ShapeDtypeStruct((64, 48, 128), jnp.bfloat16),
            jax.ShapeDtypeStruct((64, 32, 128), jnp.float32),
        ),
        in_specs=[hbm, hbm] + [vmem] * 5,
        out_specs=(vmem, vmem, vmem),
        scratch_shapes=[
            pltpu.VMEM((8, C, 9 * C), jnp.bfloat16),
            pltpu.VMEM((2, ROWS * 64, C), jnp.bfloat16),
            pltpu.VMEM((2, C, 256), jnp.bfloat16),
            pltpu.VMEM((2, 256, C), jnp.bfloat16),
            dma, dma, dma((N_SENDS,)), dma((6,)), dma((2, 2)), dma((2, 2)), dma((2, 3)), dma((2, 3)), dma((4,)),
            dma((16,)), dma((2, 16)), dma, dma((16,)), dma((2, 16)), dma, dma, dma((2,)),
        ],
        compiler_params=pltpu.CompilerParams(
            collective_id=0, has_side_effects=True, vmem_limit_bytes=40 * 2**20
        ),
        cost_estimate=pl.CostEstimate(flops=10**10, bytes_accessed=10**7, transcendentals=0),
    )(image, conv_weight, class_weight, feats, pixel, pillar, counts)


SLOTS = 128
GROUP = 16
LANES = 256


def point_kernel(points, table, wk, bev, head, out, place, packed, pooled):
    w = lax.axis_index("wide")
    first_cell = ((w - 1) * 128).astype(jnp.float32)
    one, zero = jnp.float32(1.0), jnp.float32(0.0)

    def iota(shape, dim):
        return lax.broadcasted_iota(jnp.int32, shape, dim).astype(jnp.float32)

    def where_bf16(mask):
        return jnp.where(mask, one, zero).astype(jnp.bfloat16)

    def split(value):
        high = value.astype(jnp.bfloat16)
        return high, (value - high.astype(jnp.float32)).astype(jnp.bfloat16)

    row_i = lax.broadcasted_iota(jnp.int32, (128, 128), 0)
    col_i = lax.broadcasted_iota(jnp.int32, (128, 128), 1)
    up_to = where_bf16(row_i <= col_i)
    row_j = lax.broadcasted_iota(jnp.int32, (64, 64), 0)
    col_j = lax.broadcasted_iota(jnp.int32, (64, 64), 1)
    before = where_bf16((row_j // GROUP == col_j // GROUP) & (col_j < row_j))
    all_ones = jnp.ones((128, 128), jnp.bfloat16)
    slot_row = iota((SLOTS, 128), 0)
    low_row = iota((128, LANES), 0)
    quarter_row = lax.broadcasted_iota(jnp.int32, (48, LANES), 0) // 11
    quarter_row = quarter_row.astype(jnp.float32)
    class_i = lax.broadcasted_iota(jnp.int32, (16, 48), 0)
    class_j = lax.broadcasted_iota(jnp.int32, (16, 48), 1)
    to_class = where_bf16((class_j % 11 == class_i) & (class_j < 44))
    wk_high, wk_low = split(wk[...])
    wk_both = jnp.concatenate([wk_high, wk_low], axis=0)
    column = lax.broadcasted_iota(jnp.int32, (128, 1), 0)

    def frame(f, carry):
        most = zero
        for h in range(2):
            cell = points[pl.ds((2 * f + h) * 8 + 5, 64, stride=32), :] - first_cell
            mine = (cell >= 0.0) & (cell < 384.0)
            mine_16 = where_bf16(mine)
            inside = jnp.dot(mine_16, up_to, preferred_element_type=jnp.float32)
            row_sum = jnp.dot(mine_16, all_ones, preferred_element_type=jnp.float32)
            ahead = jnp.dot(before, row_sum.astype(jnp.bfloat16), preferred_element_type=jnp.float32)
            place[h] = jnp.where(mine, inside - 1.0 + ahead, -1.0)
            most = jnp.maximum(most, jnp.max(row_sum + ahead))
        passes = (most.astype(jnp.int32) + SLOTS - 1) // SLOTS
        pooled[...] = jnp.zeros_like(pooled)

        def one_pass(number, inner):
            slot = slot_row + (number * SLOTS).astype(jnp.float32)

            def group(g, state):
                h, first = g // 4, pl.multiple_of(g % 4 * GROUP, GROUP)
                places = place[h, pl.ds(first, GROUP), :]
                data, picks = [], []
                for i in range(GROUP):
                    rows = points[pl.ds(pl.multiple_of((first + i) * 32 + (2 * f + h) * 8, 8), 8), :]
                    high, low = split(rows)
                    data.append(jnp.concatenate([high.astype(jnp.float32), low.astype(jnp.float32)], axis=0))
                    picks.append(where_bf16(slot == places[i : i + 1, :]))
                chosen = lax.dot_general(
                    jnp.concatenate(data, axis=1).astype(jnp.bfloat16), jnp.concatenate(picks, axis=1),
                    (((1,), (1,)), ((), ())), preferred_element_type=jnp.float32,
                )
                packed[g] = chosen
                return state

            lax.fori_loop(0, 8, group, 0)

            def lanes(s, state):
                chosen = jnp.concatenate([packed[2 * s], packed[2 * s + 1]], axis=1)
                value = chosen[:8] + chosen[8:]
                pixel, cell, used = value[4:5], value[5:6] - first_cell, value[6:7]
                block = jnp.floor(pixel * (1.0 / 128.0))
                low = pixel - 128.0 * block
                pair = jnp.floor(block * 0.25)
                quarter = block - 4.0 * pair
                of_frame = jnp.concatenate([table[2 * i + f] for i in range(32)], axis=0)
                read = jnp.dot(of_frame, where_bf16(low_row == low), preferred_element_type=jnp.float32)
                total = jnp.zeros((48, LANES), jnp.float32)
                for i in range(32):
                    total = total + jnp.where(pair == float(i), read[48 * i : 48 * i + 48], 0.0)
                total = jnp.where(quarter_row == quarter, total, 0.0)
                painted = jnp.dot(to_class, total.astype(jnp.bfloat16), preferred_element_type=jnp.float32)
                gate = jax.nn.sigmoid(painted)
                gate_high, gate_low = split(gate)
                features = jnp.concatenate([chosen.astype(jnp.bfloat16), gate_high, gate_low], axis=0)
                both = jnp.dot(wk_both, features, preferred_element_type=jnp.float32)
                hidden = jnp.maximum(both[:64] + both[64:], 0.0)
                row = jnp.floor(cell * (1.0 / 128.0))
                col = cell - 128.0 * row
                row = jnp.where(used > 0.5, row, -1.0)
                by_row = jnp.concatenate(
                    [jnp.where(row == float(r), hidden, 0.0) for r in range(3)], axis=0
                ).astype(jnp.bfloat16)
                pooled[...] += lax.dot_general(
                    where_bf16(low_row == col), by_row, (((1,), (1,)), ((), ())),
                    preferred_element_type=jnp.float32,
                )
                return state

            lax.fori_loop(0, 8 * SLOTS // LANES, lanes, 0)
            return inner

        lax.fori_loop(0, passes, one_pass, 0)
        grid = pooled[...]
        total = None
        for d in range(3):
            if d == 0:
                moved = jnp.where(column >= 1, pltpu.roll(grid, 1, 0), 0.0)
            elif d == 2:
                moved = jnp.where(column < 127, pltpu.roll(grid, 127, 0), 0.0)
            else:
                moved = grid
            weight = jnp.concatenate([bev[(3 * r + d) * 64 : (3 * r + d + 1) * 64, :] for r in range(3)], axis=0)
            part = jnp.dot(moved.astype(jnp.bfloat16), weight, preferred_element_type=jnp.float32)
            total = part if total is None else total + part
        feature = jnp.maximum(total, 0.0).astype(jnp.bfloat16)
        out[f] = jnp.dot(feature, head[...], preferred_element_type=jnp.float32)
        return carry

    lax.fori_loop(0, 2, frame, 0)


def point_part(points, table, wk, bev, head):
    vmem = pl.BlockSpec(memory_space=pltpu.VMEM)
    return pl.pallas_call(
        point_kernel,
        name="point_part",
        out_shape=jax.ShapeDtypeStruct((2, 128, 20), jnp.float32),
        in_specs=[vmem] * 5,
        out_specs=vmem,
        scratch_shapes=[
            pltpu.VMEM((2, 64, 128), jnp.float32),
            pltpu.VMEM((8, 16, SLOTS), jnp.float32),
            pltpu.VMEM((128, 192), jnp.float32),
        ],
        compiler_params=pltpu.CompilerParams(vmem_limit_bytes=40 * 2**20),
        cost_estimate=pl.CostEstimate(flops=10**9, bytes_accessed=3 * 10**6, transcendentals=10**5),
    )(points, table, wk, bev, head)


def local(
    image,
    conv_weight,
    class_weight,
    point_feats,
    pixel_index,
    pillar_index,
    point_counts,
    pillar_weight,
    bev_weight,
    head_weight,
):
    t = lax.axis_index("wide") % 2
    sc, table, points = image_part(
        image, conv_weight, class_weight, point_feats, pixel_index, pillar_index, point_counts
    )
    own = lax.dynamic_slice_in_dim(sc[:, :44].reshape(2, 4, 11, 128), 2 * t, 2, 1)
    scores = own.transpose(0, 2, 1, 3).reshape(2, 11, 256)
    raw, gates = pillar_weight[:, :4], jnp.pad(pillar_weight[:, 4:], ((0, 0), (0, 5)))
    raw = jnp.pad(raw, ((0, 0), (0, 4)))
    wk = jnp.concatenate([raw, raw, gates, gates], axis=1)
    detections = point_part(points.reshape(64 * 32, 128), table, wk, bev_weight, head_weight)
    return (detections, scores)


def solution(mesh):
    placed = (
        P(None, None, "wide"),
        P("phase", None, None),
        P(),
        P("phase", None, "wide"),
        P("phase", "wide"),
        P("phase", "wide"),
        P("phase", "wide"),
        P(),
        P(),
        P(),
    )
    return jax.shard_map(
        local,
        mesh=mesh,
        in_specs=placed,
        out_specs=(P("phase", "wide", None), P("phase", None, "wide")),
        check_vma=False,
    )
```

```python
import functools

import jax
import jax.numpy as jnp
from jax import lax
from jax.experimental import pallas as pl
from jax.experimental.pallas import tpu as pltpu
from jax.sharding import PartitionSpec as P

C = 256
ROWS = 24
MOST_ROWS = 12
MESH = pl.DeviceIdType.MESH
NEAR = (4, -4, 3, -3, 2, -2, 1, -1)
EARLY = (0, 4, -4, 1, -1, 2, -2, 3, -3)
LATE = (5, -5, 6, -6, 7, -7, 8)


SLOTS = 128
GROUP = 16
LANES = 256


def iota(shape, dim):
    return lax.broadcasted_iota(jnp.int32, shape, dim).astype(jnp.float32)


def where_bf16(mask):
    return jnp.where(mask, jnp.float32(1.0), jnp.float32(0.0)).astype(jnp.bfloat16)


def split(value):
    high = value.astype(jnp.bfloat16)
    return high, (value - high.astype(jnp.float32)).astype(jnp.bfloat16)


def find_places(points, place, f, first_cell):
    row_i = lax.broadcasted_iota(jnp.int32, (128, 128), 0)
    col_i = lax.broadcasted_iota(jnp.int32, (128, 128), 1)
    up_to = where_bf16(row_i <= col_i)
    row_j = lax.broadcasted_iota(jnp.int32, (64, 64), 0)
    col_j = lax.broadcasted_iota(jnp.int32, (64, 64), 1)
    before = where_bf16((row_j // GROUP == col_j // GROUP) & (col_j < row_j))
    all_ones = jnp.ones((128, 128), jnp.bfloat16)
    for h in range(2):
        cell = points[pl.ds((2 * f + h) * 8 + 5, 64, stride=32), :] - first_cell
        mine = (cell >= 0.0) & (cell < 384.0)
        mine_16 = where_bf16(mine)
        inside = jnp.dot(mine_16, up_to, preferred_element_type=jnp.float32)
        row_sum = jnp.dot(mine_16, all_ones, preferred_element_type=jnp.float32)
        ahead = jnp.dot(before, row_sum.astype(jnp.bfloat16), preferred_element_type=jnp.float32)
        place[2 * f + h] = jnp.where(mine, inside - 1.0 + ahead, -1.0)


def pack_group(points, place, packed, f, g, first_slot, where):
    h, first = g // 4, pl.multiple_of(g % 4 * GROUP, GROUP)
    slot = iota((SLOTS, 128), 0) + first_slot
    places = place[2 * f + h, pl.ds(first, GROUP), :]
    data, picks = [], []
    for i in range(GROUP):
        rows = points[pl.ds(pl.multiple_of((first + i) * 32 + (2 * f + h) * 8, 8), 8), :]
        high, low = split(rows)
        data.append(jnp.concatenate([high.astype(jnp.float32), low.astype(jnp.float32)], axis=0))
        picks.append(where_bf16(slot == places[i : i + 1, :]))
    packed[where] = lax.dot_general(
        jnp.concatenate(data, axis=1).astype(jnp.bfloat16), jnp.concatenate(picks, axis=1),
        (((1,), (1,)), ((), ())), preferred_element_type=jnp.float32,
    )


def layers(act, weights, numbers, top_row):
    for number in numbers:
        now, later = number % 2, (number + 1) % 2
        rows = 22 - 2 * number
        half = rows if rows <= MOST_ROWS else (rows + 1) // 2
        for first in range(0, rows, half):
            count = min(half, rows - first) * 64
            start = (number + 1 + first) * 64
            column = lax.broadcasted_iota(jnp.int32, (count, 1), 0) % 64
            row = lax.broadcasted_iota(jnp.int32, (count, 1), 0) // 64 + (top_row + number + 1 + first)
            lhs = jnp.concatenate([act[now, pl.ds(start + 64 * r, count), :] for r in (-1, 0, 1)], axis=1)

            def part(tap):
                rhs = jnp.concatenate(
                    [weights[number, :, (3 * r + tap) * C : (3 * r + tap + 1) * C] for r in range(3)], axis=1
                )
                return lax.dot_general(lhs, rhs, (((1,), (1,)), ((), ())), preferred_element_type=jnp.float32)

            total = part(1)
            total = total + jnp.where(column >= 1, pltpu.roll(part(0), 1, 0), 0.0)
            total = total + jnp.where(column < 63, pltpu.roll(part(2), count - 1, 0), 0.0)
            new = act[now, pl.ds(start, count), :].astype(jnp.float32) + jnp.maximum(total, 0.0)
            new = jnp.where((row >= 0) & (row < 256), new, 0.0)
            act[later, pl.ds(start, count), :] = new.astype(jnp.bfloat16)


def image_kernel(
    image, w_own, class_weight_h, feats_h, pixel_h, pillar_h, counts_h, sc, table, points, packed, place, weights, act, raw, img,
    class_weight, feats, pixel, pillar, counts, own_sem, raw_sem, in_sem, send_sem, h_sem, y1_sem, y2_sem, x1_sem, x2_sem, d_sem, tz_sem, tx_sem, tf_sem,
    pz_sem, px_sem, pf_sem, s_sem, ag_send,
):
    p = lax.axis_index("phase")
    w = lax.axis_index("wide")
    y, c = p // 2, p % 2
    x, z = w // 16, w % 16
    k, t = w // 2, w % 2
    top_row = 8 * k - 8

    def at(phase, wide):
        return {"phase": phase, "wide": wide}

    def y_dev(step):
        return at(2 * ((y + step + 4) % 4) + c, w)

    def x_dev(step):
        return at(p, 16 * ((x + step + 4) % 4) + z)

    def z_dev(step):
        return at(p, 16 * x + (z + step + 16) % 16)

    partner = at(2 * y + 1 - c, w)
    sibling = at(p, 2 * k + 1 - t)
    halo_peers = [(d, f) for d in (-1, 1) for f in (0, 1)]

    raw_copy = pltpu.make_async_copy(image.at[pl.ds(2 * p, 2)], raw, raw_sem)
    raw_copy.start()
    own_copy = pltpu.make_async_copy(w_own.at[0], weights.at[p], own_sem)
    own_copy.start()
    small = [
        pltpu.make_async_copy(src, dst, in_sem.at[i])
        for i, (src, dst) in enumerate(
            ((feats_h, feats), (pixel_h, pixel), (pillar_h, pillar), (counts_h, counts), (class_weight_h, class_weight))
        )
    ]
    for copy in small:
        copy.start()
    barrier = pltpu.get_barrier_semaphore()
    peers = [y_dev(1), y_dev(-1), partner, sibling]
    peers += [x_dev(1), x_dev(-1)] + [z_dev(d) for d in NEAR]
    peers += [at(p, (2 * (k + d) + f + 64) % 64) for d, f in halo_peers]
    for peer in peers:
        pl.semaphore_signal(barrier, inc=1, device_id=peer, device_id_type=MESH)
    for copy in small:
        copy.wait()
    lane = lax.broadcasted_iota(jnp.int32, (1, 256), 1)
    for f in range(2):
        cell = jnp.where(lane < counts[:, f : f + 1], pillar[f : f + 1, :], -1024).astype(jnp.float32)
        where = pixel[f : f + 1, :].astype(jnp.float32)
        for h in range(2):
            first = 32 * w + (2 * f + h) * 8
            points[pl.ds(first, 4), :] = feats[f, :, 128 * h : 128 * h + 128]
            points[pl.ds(first + 4, 1), :] = where[:, 128 * h : 128 * h + 128]
            points[pl.ds(first + 5, 1), :] = cell[:, 128 * h : 128 * h + 128]
            points[pl.ds(first + 6, 2), :] = jnp.ones((2, 128), jnp.float32)
    raw_copy.wait()
    for f in range(2):
        img[f] = jnp.swapaxes(raw[f], 0, 1)
    pl.semaphore_wait(barrier, len(peers))

    sends = []

    def send(src, dst, recv, device):
        number = len(sends)
        copy = pltpu.make_async_remote_copy(
            src_ref=src, dst_ref=dst, send_sem=send_sem.at[number], recv_sem=recv,
            device_id=device, device_id_type=MESH,
        )
        copy.start()
        sends.append(copy)

    def arrived(ref, recv):
        pltpu.make_async_remote_copy(
            src_ref=ref, dst_ref=ref, send_sem=send_sem.at[0], recv_sem=recv,
            device_id=partner, device_id_type=MESH,
        ).wait_recv()

    def block(j):
        return act.at[0, pl.ds(pl.multiple_of(j * 256, 256), 256), :]

    send(img.at[1 - t], block(2 + t), h_sem.at[2 + t], sibling)
    for d, f in halo_peers:
        send(img.at[f], block(2 - 2 * d + t), h_sem.at[2 - 2 * d + t], at(p, (2 * (k + d) + f + 64) % 64))

    def post(src, sem, number, device):
        pltpu.make_async_remote_copy(
            src_ref=src, dst_ref=src, send_sem=ag_send.at[number], recv_sem=sem,
            device_id=device, device_id_type=MESH,
        ).start()

    class Spread:
        def __init__(self, ref, rows, z_sem, x_sem, f_sem, number):
            self.ref, self.rows, self.number = ref, rows, number
            self.z_sem, self.x_sem, self.f_sem = z_sem, x_sem, f_sem

        def block(self, d, column=0):
            return self.some(16 * ((x + column + 4) % 4) + (z - d + 16) % 16, 1)

        def some(self, first, count):
            return self.ref.at[pl.ds(pl.multiple_of(self.rows * first, self.rows), self.rows * count)]

        def z_first(self):
            for d in NEAR:
                post(self.block(0), self.z_sem.at[d % 16], self.number, z_dev(d))

        def z_wait(self, d):
            arrived(self.block(d), self.z_sem.at[d % 16])

        def z_second(self):
            for d in (4, -4):
                self.z_wait(d)
                for e in (4, 3, 2, 1) if d > 0 else (-3, -2, -1):
                    post(self.block(d), self.z_sem.at[(d + e) % 16], self.number, z_dev(e))

        def x_first(self, d):
            for side in range(2):
                post(self.block(d), self.x_sem.at[side, d % 16], self.number, x_dev(1 - 2 * side))

        def x_second(self, d):
            for side in range(2):
                step = 1 - 2 * side
                arrived(self.block(d, -step), self.x_sem.at[side, d % 16])
                if d % 2 == side:
                    post(self.block(d, -step), self.f_sem, self.number, x_dev(step))

        def last(self):
            arrived(self.some(16 * ((x + 2) % 4), 16), self.f_sem)

        def sent(self):
            pltpu.make_async_remote_copy(
                src_ref=self.some(0, 63), dst_ref=self.some(0, 63),
                send_sem=ag_send.at[self.number], recv_sem=own_sem, device_id=partner, device_id_type=MESH,
            ).wait_send()

    spread_points = Spread(points, 32, pz_sem, px_sem, pf_sem, 0)
    spread_table = Spread(table, 48, tz_sem, tx_sem, tf_sem, 1)

    def q_cols(layer, owner, first=0, tiles=3):
        return weights.at[layer, :, pl.ds(pl.multiple_of(768 + 384 * owner + 128 * first, 128), 128 * tiles)]

    def a_cols(layer, half):
        return weights.at[layer, :, pl.ds(384 * half, 384)]

    def layer_of(step):
        return 2 * ((y + step + 8) % 4) + c

    q_parts = ((0, 2), (2, 1))
    sign = 1 - 2 * c
    steps = (sign, -sign)
    near = [layer_of(-sign), layer_of(sign)]
    far = layer_of(2)
    soon_step = 1 - 2 * (((y + 1) // 2) % 2)
    soon = (1 + soon_step * sign) // 2
    late = 1 - soon
    soon_layer, late_layer = layer_of(soon_step), layer_of(-soon_step)

    def x_first(layer, j):
        for d in range(2):
            send(q_cols(layer, x), q_cols(layer, x), x1_sem.at[d, j], x_dev(steps[d]))

    def x_second(layer, j):
        for d in range(2):
            source = (x - steps[d] + 4) % 4
            arrived(q_cols(layer, source), x1_sem.at[d, j])
            part = q_cols(layer, source, *q_parts[d])
            send(part, part, x2_sem.at[d, j], x_dev(steps[d]))

    def x_done(layer, j):
        for d in range(2):
            arrived(q_cols(layer, (x + 2) % 4, *q_parts[d]), x2_sem.at[d, j])

    def hand_over(layer, half):
        part = weights.at[layer, :, pl.ds(768 * half, 768 + 768 * half)]
        send(part, part, d_sem.at[layer // 2, half], partner)

    def taken_over(number):
        @pl.when(c == 1 - number % 2)
        def _():
            for half in range(2):
                arrived(weights.at[number, :, pl.ds(768 * half, 768 + 768 * half)], d_sem.at[number // 2, half])

    own_copy.wait()
    for d in range(2):
        send(q_cols(p, x), q_cols(p, x), y1_sem.at[d, 0], y_dev(steps[d]))
    for d in range(2):
        send(a_cols(p, d), a_cols(p, d), y1_sem.at[d, 1], y_dev(steps[d]))
    hand_over(p, 0)
    hand_over(p, 1)
    spread_points.z_first()
    for d in range(2):
        arrived(q_cols(near[d], x), y1_sem.at[d, 0])
        part = q_cols(near[d], x, *q_parts[d])
        send(part, part, y2_sem.at[d, 0], y_dev(steps[d]))
    x_first(soon_layer, soon)
    for d in range(2):
        arrived(a_cols(near[d], d), y1_sem.at[d, 1])
        send(a_cols(near[d], d), a_cols(near[d], d), y2_sem.at[d, 1], y_dev(steps[d]))
        send(a_cols(p, 1 - d), a_cols(p, 1 - d), y1_sem.at[d, 2], y_dev(steps[d]))
    for d in range(2):
        arrived(q_cols(far, x, *q_parts[d]), y2_sem.at[d, 0])
    x_first(far, 2)
    x_second(soon_layer, soon)
    x_second(far, 2)
    x_first(late_layer, late)
    for d in range(2):
        arrived(a_cols(far, d), y2_sem.at[d, 1])
    hand_over(far, 0)
    spread_points.z_second()
    for d in range(2):
        arrived(a_cols(near[d], 1 - d), y1_sem.at[d, 2])
    hand_over(soon_layer, 0)
    hand_over(late_layer, 0)
    x_done(soon_layer, soon)
    hand_over(soon_layer, 1)
    x_done(far, 2)
    hand_over(far, 1)

    act[0, pl.ds(pl.multiple_of((2 + t) * 256, 256), 256), :] = img[t]
    for j in (0, 1, 4, 5):
        arrived(block(j), h_sem.at[j])
    arrived(block(3 - t), h_sem.at[3 - t])

    @pl.when(k == 0)
    def _():
        act[0, pl.ds(0, 512), :] = jnp.zeros((512, C), jnp.bfloat16)

    @pl.when(k == 31)
    def _():
        act[0, pl.ds(1024, 512), :] = jnp.zeros((512, C), jnp.bfloat16)

    def layer(number):
        taken_over(number)
        layers(act, weights, (number,), top_row)

    layer(0)
    layer(1)
    x_second(late_layer, late)
    for d in EARLY + LATE:
        if d not in (0, 4, -4):
            spread_points.z_wait(d)
        spread_points.x_first(d)
    layer(2)
    x_done(late_layer, late)
    hand_over(late_layer, 1)
    layer(3)
    layer(4)
    for d in EARLY + LATE:
        spread_points.x_second(d)
    layer(5)
    layer(6)
    layer(7)

    row_i = lax.broadcasted_iota(jnp.int32, (48, 11), 0)
    row_j = lax.broadcasted_iota(jnp.int32, (48, 11), 1)
    placed = []
    for q in range(4):
        here = jnp.where(row_i == row_j + 11 * q, 1.0, 0.0).astype(jnp.bfloat16)
        placed.append(
            jnp.dot(here, class_weight[...], preferred_element_type=jnp.float32).astype(jnp.bfloat16)
        )
    total = None
    for q in range(4):
        part = lax.dot_general(
            placed[q], act[0, pl.ds(512 + 128 * q, 128), :], (((1,), (1,)), ((), ())),
            preferred_element_type=jnp.float32,
        )
        total = part if total is None else total + part
    table[pl.ds(pl.multiple_of(48 * w, 48), 48), :] = total.astype(jnp.bfloat16)
    sc[t] = total
    spread_table.z_first()
    spread_table.x_first(0)
    send(sc.at[t], sc.at[t], s_sem, sibling)
    spread_points.last()
    first_cell = ((w - 1) * 128).astype(jnp.float32)
    for f in range(2):
        find_places(points, place, f, first_cell)

    def pack(first, last):
        def one(g, state):
            pack_group(points, place, packed, g // 8, g % 8, 0.0, g)
            return state

        lax.fori_loop(first, last, one, 0)

    pack(0, 4)
    spread_table.z_second()
    spread_table.x_first(4)
    spread_table.x_first(-4)
    for d in (1, -1, 2, -2, 3, -3):
        spread_table.z_wait(d)
        spread_table.x_first(d)
    pack(4, 8)
    for d in EARLY:
        spread_table.x_second(d)
    for d in LATE:
        spread_table.z_wait(d)
        spread_table.x_first(d)
    pack(8, 16)
    for d in LATE:
        spread_table.x_second(d)
    spread_points.sent()
    spread_table.last()
    spread_table.sent()
    arrived(sc.at[1 - t], s_sem)
    for copy in sends:
        copy.wait_send()


N_SENDS = 48


def image_part(image, conv_weight, class_weight, feats, pixel, pillar, counts):
    vmem = pl.BlockSpec(memory_space=pltpu.VMEM)
    hbm = pl.BlockSpec(memory_space=pltpu.HBM)
    dma = pltpu.SemaphoreType.DMA
    operands = (image, conv_weight, class_weight, feats, pixel, pillar, counts.reshape(1, 2))
    operands = [pltpu.with_memory_space_constraint(o, pltpu.HBM) for o in operands]
    return pl.pallas_call(
        image_kernel,
        name="image_part",
        out_shape=(
            jax.ShapeDtypeStruct((2, 48, 128), jnp.float32),
            jax.ShapeDtypeStruct((64 * 48, 128), jnp.bfloat16),
            jax.ShapeDtypeStruct((64 * 32, 128), jnp.float32),
            jax.ShapeDtypeStruct((16, 16, SLOTS), jnp.float32),
            jax.ShapeDtypeStruct((4, 64, 128), jnp.float32),
        ),
        in_specs=[hbm] * 7,
        out_specs=(vmem,) * 5,
        scratch_shapes=[
            pltpu.VMEM((8, C, 9 * C), jnp.bfloat16),
            pltpu.VMEM((2, ROWS * 64, C), jnp.bfloat16),
            pltpu.VMEM((2, C, 256), jnp.bfloat16),
            pltpu.VMEM((2, 256, C), jnp.bfloat16),
            pltpu.VMEM((11, C), jnp.bfloat16),
            pltpu.VMEM((2, 4, 256), jnp.float32),
            pltpu.VMEM((2, 256), jnp.int32),
            pltpu.VMEM((2, 256), jnp.int32),
            pltpu.VMEM((1, 2), jnp.int32),
            dma, dma, dma((5,)), dma((N_SENDS,)), dma((6,)), dma((2, 3)), dma((2, 2)), dma((2, 3)), dma((2, 3)), dma((4, 2)),
            dma((16,)), dma((2, 16)), dma, dma((16,)), dma((2, 16)), dma, dma, dma((2,)),
        ],
        compiler_params=pltpu.CompilerParams(
            collective_id=0, has_side_effects=True, vmem_limit_bytes=40 * 2**20
        ),
        cost_estimate=pl.CostEstimate(flops=10**10, bytes_accessed=10**7, transcendentals=0),
    )(*operands)


def point_kernel(points, table, packed_first, place, sc, wk, bev, head, out, scores, packed, pooled, found):
    w = lax.axis_index("wide")
    first_cell = ((w - 1) * 128).astype(jnp.float32)
    low_row = iota((128, LANES), 0)
    quarter_row = lax.broadcasted_iota(jnp.int32, (48, LANES), 0) // 11
    quarter_row = quarter_row.astype(jnp.float32)
    class_i = lax.broadcasted_iota(jnp.int32, (16, 48), 0)
    class_j = lax.broadcasted_iota(jnp.int32, (16, 48), 1)
    to_class = where_bf16((class_j % 11 == class_i) & (class_j < 44))
    wk_high, wk_low = split(wk[...])
    wk_both = jnp.concatenate([wk_high, wk_low], axis=0)
    column = lax.broadcasted_iota(jnp.int32, (128, 1), 0)

    def frame(f, carry):
        most = jnp.max(jnp.maximum(place[2 * f], place[2 * f + 1])) + 1.0
        passes = (most.astype(jnp.int32) + SLOTS - 1) // SLOTS
        packed[...] = packed_first[pl.ds(8 * f, 8)]
        pooled[...] = jnp.zeros_like(pooled)

        def one_pass(number, inner):
            @pl.when(number > 0)
            def _():
                def group(g, state):
                    pack_group(points, place, packed, f, g, (number * SLOTS).astype(jnp.float32), g)
                    return state

                lax.fori_loop(0, 8, group, 0)

            def lanes(s, state):
                chosen = jnp.concatenate([packed[2 * s], packed[2 * s + 1]], axis=1)
                value = chosen[:8] + chosen[8:]
                pixel, cell, used = value[4:5], value[5:6] - first_cell, value[6:7]
                block = jnp.floor(pixel * (1.0 / 128.0))
                low = pixel - 128.0 * block
                pair = jnp.floor(block * 0.25)
                quarter = block - 4.0 * pair
                of_frame = jnp.concatenate([table[pl.ds(pl.multiple_of((2 * i + f) * 48, 48), 48), :] for i in range(32)], axis=0)
                read = jnp.dot(of_frame, where_bf16(low_row == low), preferred_element_type=jnp.float32)
                total = jnp.zeros((48, LANES), jnp.float32)
                for i in range(32):
                    total = total + jnp.where(pair == float(i), read[48 * i : 48 * i + 48], 0.0)
                total = jnp.where(quarter_row == quarter, total, 0.0)
                painted = jnp.dot(to_class, total.astype(jnp.bfloat16), preferred_element_type=jnp.float32)
                gate = jax.nn.sigmoid(painted)
                gate_high, gate_low = split(gate)
                features = jnp.concatenate([chosen.astype(jnp.bfloat16), gate_high, gate_low], axis=0)
                both = jnp.dot(wk_both, features, preferred_element_type=jnp.float32)
                hidden = jnp.maximum(both[:64] + both[64:], 0.0)
                row = jnp.floor(cell * (1.0 / 128.0))
                col = cell - 128.0 * row
                row = jnp.where(used > 0.5, row, -1.0)
                by_row = jnp.concatenate(
                    [jnp.where(row == float(r), hidden, 0.0) for r in range(3)], axis=0
                ).astype(jnp.bfloat16)
                pooled[...] += lax.dot_general(
                    where_bf16(low_row == col), by_row, (((1,), (1,)), ((), ())),
                    preferred_element_type=jnp.float32,
                )
                return state

            lax.fori_loop(0, 8 * SLOTS // LANES, lanes, 0)
            return inner

        lax.fori_loop(0, passes, one_pass, 0)
        grid = pooled[...]
        total = None
        for d in range(3):
            if d == 0:
                moved = jnp.where(column >= 1, pltpu.roll(grid, 1, 0), 0.0)
            elif d == 2:
                moved = jnp.where(column < 127, pltpu.roll(grid, 127, 0), 0.0)
            else:
                moved = grid
            weight = jnp.concatenate([bev[(3 * r + d) * 64 : (3 * r + d + 1) * 64, :] for r in range(3)], axis=0)
            part = jnp.dot(moved.astype(jnp.bfloat16), weight, preferred_element_type=jnp.float32)
            total = part if total is None else total + part
        feature = jnp.maximum(total, 0.0).astype(jnp.bfloat16)
        found[f] = lax.dot_general(
            head[...], feature, (((1,), (1,)), ((), ())), preferred_element_type=jnp.float32
        )
        return carry

    lax.fori_loop(0, 2, frame, 0)
    for f in range(2):
        out[:, f, :] = found[f]
        for half in range(2):
            even, odd = sc[f, 11 * half : 11 * half + 11, :], sc[f, 11 * half + 22 : 11 * half + 33, :]
            scores[:, f, 128 * half : 128 * half + 128] = jnp.where(w % 2 == 0, even, odd)


def point_part(points, table, packed, place, sc, wk, bev, head):
    vmem = pl.BlockSpec(memory_space=pltpu.VMEM)
    return pl.pallas_call(
        point_kernel,
        name="point_part",
        out_shape=(
            jax.ShapeDtypeStruct((20, 2, 128), jnp.float32),
            jax.ShapeDtypeStruct((11, 2, 256), jnp.float32),
        ),
        in_specs=[vmem] * 8,
        out_specs=(vmem, vmem),
        scratch_shapes=[
            pltpu.VMEM((8, 16, SLOTS), jnp.float32),
            pltpu.VMEM((128, 192), jnp.float32),
            pltpu.VMEM((2, 20, 128), jnp.float32),
        ],
        compiler_params=pltpu.CompilerParams(vmem_limit_bytes=40 * 2**20),
        cost_estimate=pl.CostEstimate(flops=10**9, bytes_accessed=3 * 10**6, transcendentals=10**5),
    )(points, table, packed, place, sc, wk, bev, head)


def local(
    image,
    conv_weight,
    class_weight,
    point_feats,
    pixel_index,
    pillar_index,
    point_counts,
    pillar_weight,
    bev_weight,
    head_weight,
):
    sc, table, points, packed, place = image_part(
        image, conv_weight, class_weight, point_feats, pixel_index, pillar_index, point_counts
    )
    raw, gates = pillar_weight[:, :4], jnp.pad(pillar_weight[:, 4:], ((0, 0), (0, 5)))
    raw = jnp.pad(raw, ((0, 0), (0, 4)))
    wk = jnp.concatenate([raw, raw, gates, gates], axis=1)
    detections, scores = point_part(points, table, packed, place, sc, wk, bev_weight, head_weight.T)
    return (detections.transpose(1, 2, 0), scores.transpose(1, 0, 2))


def solution(mesh):
    placed = (
        P(None, None, "wide"),
        P("phase", None, None),
        P(),
        P("phase", None, "wide"),
        P("phase", "wide"),
        P("phase", "wide"),
        P("phase", "wide"),
        P(),
        P(),
        P(),
    )
    return jax.shard_map(
        local,
        mesh=mesh,
        in_specs=placed,
        out_specs=(P("phase", "wide", None), P("phase", None, "wide")),
        check_vma=False,
    )
```

```python
import functools

import jax
import jax.numpy as jnp
from jax import lax
from jax.experimental import pallas as pl
from jax.experimental.pallas import tpu as pltpu
from jax.sharding import PartitionSpec as P

C = 256
ROWS = 24
MOST_ROWS = 12
MESH = pl.DeviceIdType.MESH
NEAR = (4, -4, 3, -3, 2, -2, 1, -1)
EARLY = (0, 4, -4, 1, -1, 2, -2, 3, -3)
LATE = (5, -5, 6, -6, 7, -7, 8)


SLOTS = 128
GROUP = 16
LANES = 1024


def iota(shape, dim):
    return lax.broadcasted_iota(jnp.int32, shape, dim).astype(jnp.float32)


def where_bf16(mask):
    return jnp.where(mask, jnp.float32(1.0), jnp.float32(0.0)).astype(jnp.bfloat16)


def split(value):
    high = value.astype(jnp.bfloat16)
    return high, (value - high.astype(jnp.float32)).astype(jnp.bfloat16)


def find_places(points, place, f, first_cell):
    row_i = lax.broadcasted_iota(jnp.int32, (128, 128), 0)
    col_i = lax.broadcasted_iota(jnp.int32, (128, 128), 1)
    up_to = where_bf16(row_i <= col_i)
    row_j = lax.broadcasted_iota(jnp.int32, (64, 64), 0)
    col_j = lax.broadcasted_iota(jnp.int32, (64, 64), 1)
    before = where_bf16((row_j // GROUP == col_j // GROUP) & (col_j < row_j))
    all_ones = jnp.ones((128, 128), jnp.bfloat16)
    for h in range(2):
        cell = points[pl.ds((2 * f + h) * 8 + 5, 64, stride=32), :] - first_cell
        mine = (cell >= 0.0) & (cell < 384.0)
        mine_16 = where_bf16(mine)
        inside = jnp.dot(mine_16, up_to, preferred_element_type=jnp.float32)
        row_sum = jnp.dot(mine_16, all_ones, preferred_element_type=jnp.float32)
        ahead = jnp.dot(before, row_sum.astype(jnp.bfloat16), preferred_element_type=jnp.float32)
        place[2 * f + h] = jnp.where(mine, inside - 1.0 + ahead, -1.0)


def pack_group(points, place, packed, f, g, first_slot, where):
    h, first = g // 4, pl.multiple_of(g % 4 * GROUP, GROUP)
    slot = iota((SLOTS, 128), 0) + first_slot
    places = place[2 * f + h, pl.ds(first, GROUP), :]
    data, picks = [], []
    for i in range(GROUP):
        rows = points[pl.ds(pl.multiple_of((first + i) * 32 + (2 * f + h) * 8, 8), 8), :]
        high, low = split(rows)
        data.append(jnp.concatenate([high.astype(jnp.float32), low.astype(jnp.float32)], axis=0))
        picks.append(where_bf16(slot == places[i : i + 1, :]))
    packed[where] = lax.dot_general(
        jnp.concatenate(data, axis=1).astype(jnp.bfloat16), jnp.concatenate(picks, axis=1),
        (((1,), (1,)), ((), ())), preferred_element_type=jnp.float32,
    )


def layers(act, weights, numbers, top_row):
    for number in numbers:
        now, later = number % 2, (number + 1) % 2
        rows = 22 - 2 * number
        half = rows if rows <= MOST_ROWS else (rows + 1) // 2
        for first in range(0, rows, half):
            count = min(half, rows - first) * 64
            start = (number + 1 + first) * 64
            column = lax.broadcasted_iota(jnp.int32, (count, 1), 0) % 64
            row = lax.broadcasted_iota(jnp.int32, (count, 1), 0) // 64 + (top_row + number + 1 + first)
            lhs = jnp.concatenate([act[now, pl.ds(start + 64 * r, count), :] for r in (-1, 0, 1)], axis=1)

            def part(tap):
                rhs = jnp.concatenate(
                    [weights[number, :, (3 * r + tap) * C : (3 * r + tap + 1) * C] for r in range(3)], axis=1
                )
                return lax.dot_general(lhs, rhs, (((1,), (1,)), ((), ())), preferred_element_type=jnp.float32)

            total = part(1)
            total = total + jnp.where(column >= 1, pltpu.roll(part(0), 1, 0), 0.0)
            total = total + jnp.where(column < 63, pltpu.roll(part(2), count - 1, 0), 0.0)
            new = act[now, pl.ds(start, count), :].astype(jnp.float32) + jnp.maximum(total, 0.0)
            new = jnp.where((row >= 0) & (row < 256), new, 0.0)
            act[later, pl.ds(start, count), :] = new.astype(jnp.bfloat16)


def image_kernel(
    image, w_own, class_weight_h, feats_h, pixel_h, pillar_h, counts_h, sc, table, points, packed, place, weights, act, raw, img,
    class_weight, feats, pixel, pillar, counts, own_sem, raw_sem, in_sem, send_sem, h_sem, y1_sem, y2_sem, x1_sem, x2_sem, d_sem, tz_sem, tx_sem, tf_sem,
    pz_sem, px_sem, pf_sem, s_sem, ag_send,
):
    p = lax.axis_index("phase")
    w = lax.axis_index("wide")
    y, c = p // 2, p % 2
    x, z = w // 16, w % 16
    k, t = w // 2, w % 2
    top_row = 8 * k - 8

    def at(phase, wide):
        return {"phase": phase, "wide": wide}

    def y_dev(step):
        return at(2 * ((y + step + 4) % 4) + c, w)

    def x_dev(step):
        return at(p, 16 * ((x + step + 4) % 4) + z)

    def z_dev(step):
        return at(p, 16 * x + (z + step + 16) % 16)

    partner = at(2 * y + 1 - c, w)
    sibling = at(p, 2 * k + 1 - t)
    halo_peers = [(d, f) for d in (-1, 1) for f in (0, 1)]

    raw_copy = pltpu.make_async_copy(image.at[pl.ds(2 * p, 2)], raw, raw_sem)
    raw_copy.start()
    own_copy = pltpu.make_async_copy(w_own.at[0], weights.at[p], own_sem)
    own_copy.start()
    small = [
        pltpu.make_async_copy(src, dst, in_sem.at[i])
        for i, (src, dst) in enumerate(
            ((feats_h, feats), (pixel_h, pixel), (pillar_h, pillar), (counts_h, counts), (class_weight_h, class_weight))
        )
    ]
    for copy in small:
        copy.start()
    barrier = pltpu.get_barrier_semaphore()
    peers = [y_dev(1), y_dev(-1), partner, sibling]
    peers += [x_dev(1), x_dev(-1)] + [z_dev(d) for d in NEAR]
    peers += [at(p, (2 * (k + d) + f + 64) % 64) for d, f in halo_peers]
    for peer in peers:
        pl.semaphore_signal(barrier, inc=1, device_id=peer, device_id_type=MESH)
    for copy in small:
        copy.wait()
    lane = lax.broadcasted_iota(jnp.int32, (1, 256), 1)
    for f in range(2):
        cell = jnp.where(lane < counts[:, f : f + 1], pillar[f : f + 1, :], -1024).astype(jnp.float32)
        where = pixel[f : f + 1, :].astype(jnp.float32)
        for h in range(2):
            first = 32 * w + (2 * f + h) * 8
            points[pl.ds(first, 4), :] = feats[f, :, 128 * h : 128 * h + 128]
            points[pl.ds(first + 4, 1), :] = where[:, 128 * h : 128 * h + 128]
            points[pl.ds(first + 5, 1), :] = cell[:, 128 * h : 128 * h + 128]
            points[pl.ds(first + 6, 2), :] = jnp.ones((2, 128), jnp.float32)
    raw_copy.wait()
    for f in range(2):
        img[f] = jnp.swapaxes(raw[f], 0, 1)
    pl.semaphore_wait(barrier, len(peers))

    sends = []

    def send(src, dst, recv, device):
        number = len(sends)
        copy = pltpu.make_async_remote_copy(
            src_ref=src, dst_ref=dst, send_sem=send_sem.at[number], recv_sem=recv,
            device_id=device, device_id_type=MESH,
        )
        copy.start()
        sends.append(copy)

    def arrived(ref, recv):
        pltpu.make_async_remote_copy(
            src_ref=ref, dst_ref=ref, send_sem=send_sem.at[0], recv_sem=recv,
            device_id=partner, device_id_type=MESH,
        ).wait_recv()

    def block(j):
        return act.at[0, pl.ds(pl.multiple_of(j * 256, 256), 256), :]

    send(img.at[1 - t], block(2 + t), h_sem.at[2 + t], sibling)
    for d, f in halo_peers:
        send(img.at[f], block(2 - 2 * d + t), h_sem.at[2 - 2 * d + t], at(p, (2 * (k + d) + f + 64) % 64))

    def post(src, sem, number, device):
        pltpu.make_async_remote_copy(
            src_ref=src, dst_ref=src, send_sem=ag_send.at[number], recv_sem=sem,
            device_id=device, device_id_type=MESH,
        ).start()

    class Spread:
        def __init__(self, ref, rows, z_sem, x_sem, f_sem, number):
            self.ref, self.rows, self.number = ref, rows, number
            self.z_sem, self.x_sem, self.f_sem = z_sem, x_sem, f_sem

        def block(self, d, column=0):
            return self.some(16 * ((x + column + 4) % 4) + (z - d + 16) % 16, 1)

        def some(self, first, count):
            return self.ref.at[pl.ds(pl.multiple_of(self.rows * first, self.rows), self.rows * count)]

        def z_first(self):
            for d in NEAR:
                post(self.block(0), self.z_sem.at[d % 16], self.number, z_dev(d))

        def z_wait(self, d):
            arrived(self.block(d), self.z_sem.at[d % 16])

        def z_second(self):
            for d in (4, -4):
                self.z_wait(d)
                for e in (4, 3, 2, 1) if d > 0 else (-3, -2, -1):
                    post(self.block(d), self.z_sem.at[(d + e) % 16], self.number, z_dev(e))

        def x_first(self, d):
            for side in range(2):
                post(self.block(d), self.x_sem.at[side, d % 16], self.number, x_dev(1 - 2 * side))

        def x_second(self, d):
            for side in range(2):
                step = 1 - 2 * side
                arrived(self.block(d, -step), self.x_sem.at[side, d % 16])
                if d % 2 == side:
                    post(self.block(d, -step), self.f_sem, self.number, x_dev(step))

        def last(self):
            arrived(self.some(16 * ((x + 2) % 4), 16), self.f_sem)

        def sent(self):
            pltpu.make_async_remote_copy(
                src_ref=self.some(0, 63), dst_ref=self.some(0, 63),
                send_sem=ag_send.at[self.number], recv_sem=own_sem, device_id=partner, device_id_type=MESH,
            ).wait_send()

    spread_points = Spread(points, 32, pz_sem, px_sem, pf_sem, 0)
    spread_table = Spread(table, 48, tz_sem, tx_sem, tf_sem, 1)

    def q_cols(layer, owner, first=0, tiles=3):
        return weights.at[layer, :, pl.ds(pl.multiple_of(768 + 384 * owner + 128 * first, 128), 128 * tiles)]

    def a_cols(layer, half):
        return weights.at[layer, :, pl.ds(384 * half, 384)]

    def layer_of(step):
        return 2 * ((y + step + 8) % 4) + c

    q_parts = ((0, 2), (2, 1))
    sign = 1 - 2 * c
    steps = (sign, -sign)
    near = [layer_of(-sign), layer_of(sign)]
    far = layer_of(2)
    soon_step = 1 - 2 * (((y + 1) // 2) % 2)
    soon = (1 + soon_step * sign) // 2
    late = 1 - soon
    soon_layer, late_layer = layer_of(soon_step), layer_of(-soon_step)

    def x_first(layer, j):
        for d in range(2):
            send(q_cols(layer, x), q_cols(layer, x), x1_sem.at[d, j], x_dev(steps[d]))

    def x_second(layer, j):
        for d in range(2):
            source = (x - steps[d] + 4) % 4
            arrived(q_cols(layer, source), x1_sem.at[d, j])
            part = q_cols(layer, source, *q_parts[d])
            send(part, part, x2_sem.at[d, j], x_dev(steps[d]))

    def x_done(layer, j):
        for d in range(2):
            arrived(q_cols(layer, (x + 2) % 4, *q_parts[d]), x2_sem.at[d, j])

    def hand_over(layer, half):
        part = weights.at[layer, :, pl.ds(768 * half, 768 + 768 * half)]
        send(part, part, d_sem.at[layer // 2, half], partner)

    def taken_over(number):
        @pl.when(c == 1 - number % 2)
        def _():
            for half in range(2):
                arrived(weights.at[number, :, pl.ds(768 * half, 768 + 768 * half)], d_sem.at[number // 2, half])

    own_copy.wait()
    for d in range(2):
        send(q_cols(p, x), q_cols(p, x), y1_sem.at[d, 0], y_dev(steps[d]))
    hand_over(p, 0)
    hand_over(p, 1)
    spread_points.z_first()
    for d in range(2):
        arrived(q_cols(near[d], x), y1_sem.at[d, 0])
        part = q_cols(near[d], x, *q_parts[d])
        send(part, part, y2_sem.at[d, 0], y_dev(steps[d]))
    x_first(soon_layer, soon)
    for d in range(2):
        send(a_cols(p, d), a_cols(p, d), y1_sem.at[d, 1], y_dev(steps[d]))
    for d in range(2):
        arrived(a_cols(near[d], d), y1_sem.at[d, 1])
        send(a_cols(near[d], d), a_cols(near[d], d), y2_sem.at[d, 1], y_dev(steps[d]))
        send(a_cols(p, 1 - d), a_cols(p, 1 - d), y1_sem.at[d, 2], y_dev(steps[d]))
    for d in range(2):
        arrived(q_cols(far, x, *q_parts[d]), y2_sem.at[d, 0])
    x_first(far, 2)
    x_second(soon_layer, soon)
    x_second(far, 2)
    x_first(late_layer, late)
    for d in range(2):
        arrived(a_cols(far, d), y2_sem.at[d, 1])
    hand_over(far, 0)
    spread_points.z_second()
    for d in range(2):
        arrived(a_cols(near[d], 1 - d), y1_sem.at[d, 2])
    hand_over(soon_layer, 0)
    hand_over(late_layer, 0)
    x_done(soon_layer, soon)
    hand_over(soon_layer, 1)
    x_done(far, 2)
    hand_over(far, 1)

    act[0, pl.ds(pl.multiple_of((2 + t) * 256, 256), 256), :] = img[t]
    for j in (0, 1, 4, 5):
        arrived(block(j), h_sem.at[j])
    arrived(block(3 - t), h_sem.at[3 - t])

    @pl.when(k == 0)
    def _():
        act[0, pl.ds(0, 512), :] = jnp.zeros((512, C), jnp.bfloat16)

    @pl.when(k == 31)
    def _():
        act[0, pl.ds(1024, 512), :] = jnp.zeros((512, C), jnp.bfloat16)

    def layer(number):
        taken_over(number)
        layers(act, weights, (number,), top_row)

    layer(0)
    layer(1)
    x_second(late_layer, late)
    for d in EARLY + LATE:
        if d not in (0, 4, -4):
            spread_points.z_wait(d)
        spread_points.x_first(d)
    layer(2)
    x_done(late_layer, late)
    hand_over(late_layer, 1)
    layer(3)
    layer(4)
    for d in EARLY + LATE:
        spread_points.x_second(d)
    layer(5)
    layer(6)
    layer(7)

    row_i = lax.broadcasted_iota(jnp.int32, (48, 11), 0)
    row_j = lax.broadcasted_iota(jnp.int32, (48, 11), 1)
    placed = []
    for q in range(4):
        here = jnp.where(row_i == row_j + 11 * q, 1.0, 0.0).astype(jnp.bfloat16)
        placed.append(
            jnp.dot(here, class_weight[...], preferred_element_type=jnp.float32).astype(jnp.bfloat16)
        )
    total = None
    for q in range(4):
        part = lax.dot_general(
            placed[q], act[0, pl.ds(512 + 128 * q, 128), :], (((1,), (1,)), ((), ())),
            preferred_element_type=jnp.float32,
        )
        total = part if total is None else total + part
    table[pl.ds(pl.multiple_of(48 * w, 48), 48), :] = total.astype(jnp.bfloat16)
    sc[t] = total
    spread_table.z_first()
    spread_table.x_first(0)
    send(sc.at[t], sc.at[t], s_sem, sibling)
    spread_points.last()
    first_cell = ((w - 1) * 128).astype(jnp.float32)
    for f in range(2):
        find_places(points, place, f, first_cell)

    def pack(first, last):
        def one(g, state):
            pack_group(points, place, packed, g // 8, g % 8, 0.0, g)
            return state

        lax.fori_loop(first, last, one, 0)

    pack(0, 4)
    spread_table.z_second()
    spread_table.x_first(4)
    spread_table.x_first(-4)
    for d in (1, -1, 2, -2, 3, -3):
        spread_table.z_wait(d)
        spread_table.x_first(d)
    pack(4, 8)
    for d in EARLY:
        spread_table.x_second(d)
    for d in LATE:
        spread_table.z_wait(d)
        spread_table.x_first(d)
    pack(8, 16)
    for d in LATE:
        spread_table.x_second(d)
    spread_points.sent()
    spread_table.last()
    spread_table.sent()
    arrived(sc.at[1 - t], s_sem)
    for copy in sends:
        copy.wait_send()


N_SENDS = 48


def image_part(image, conv_weight, class_weight, feats, pixel, pillar, counts):
    vmem = pl.BlockSpec(memory_space=pltpu.VMEM)
    hbm = pl.BlockSpec(memory_space=pltpu.HBM)
    dma = pltpu.SemaphoreType.DMA
    operands = (image, conv_weight, class_weight, feats, pixel, pillar, counts.reshape(1, 2))
    operands = [pltpu.with_memory_space_constraint(o, pltpu.HBM) for o in operands]
    return pl.pallas_call(
        image_kernel,
        name="image_part",
        out_shape=(
            jax.ShapeDtypeStruct((2, 48, 128), jnp.float32),
            jax.ShapeDtypeStruct((64 * 48, 128), jnp.bfloat16),
            jax.ShapeDtypeStruct((64 * 32, 128), jnp.float32),
            jax.ShapeDtypeStruct((16, 16, SLOTS), jnp.float32),
            jax.ShapeDtypeStruct((4, 64, 128), jnp.float32),
        ),
        in_specs=[hbm] * 7,
        out_specs=(vmem,) * 5,
        scratch_shapes=[
            pltpu.VMEM((8, C, 9 * C), jnp.bfloat16),
            pltpu.VMEM((2, ROWS * 64, C), jnp.bfloat16),
            pltpu.VMEM((2, C, 256), jnp.bfloat16),
            pltpu.VMEM((2, 256, C), jnp.bfloat16),
            pltpu.VMEM((11, C), jnp.bfloat16),
            pltpu.VMEM((2, 4, 256), jnp.float32),
            pltpu.VMEM((2, 256), jnp.int32),
            pltpu.VMEM((2, 256), jnp.int32),
            pltpu.VMEM((1, 2), jnp.int32),
            dma, dma, dma((5,)), dma((N_SENDS,)), dma((6,)), dma((2, 3)), dma((2, 2)), dma((2, 3)), dma((2, 3)), dma((4, 2)),
            dma((16,)), dma((2, 16)), dma, dma((16,)), dma((2, 16)), dma, dma, dma((2,)),
        ],
        compiler_params=pltpu.CompilerParams(
            collective_id=0, has_side_effects=True, vmem_limit_bytes=40 * 2**20
        ),
        cost_estimate=pl.CostEstimate(flops=10**10, bytes_accessed=10**7, transcendentals=0),
    )(*operands)


def point_kernel(points, table, packed_first, place, sc, pillar, bev, head, out, scores, packed, pooled, spare):
    w = lax.axis_index("wide")
    first_cell = ((w - 1) * 128).astype(jnp.float32)
    low_row = iota((128, LANES), 0)
    quarter_row = lax.broadcasted_iota(jnp.int32, (48, LANES), 0) // 11
    quarter_row = quarter_row.astype(jnp.float32)
    class_i = lax.broadcasted_iota(jnp.int32, (16, 48), 0)
    class_j = lax.broadcasted_iota(jnp.int32, (16, 48), 1)
    to_class = where_bf16((class_j % 11 == class_i) & (class_j < 44))
    spare[...] = jnp.zeros_like(spare)
    for first in (0, 8):
        spare[first : first + 4, :64] = pillar[:4, :]
    for first in (16, 32):
        spare[first : first + 11, :64] = pillar[4:, :]
    wk_high, wk_low = split(jnp.swapaxes(spare[...], 0, 1)[:64, :48])
    wk_both = jnp.concatenate([wk_high, wk_low], axis=0)
    column = lax.broadcasted_iota(jnp.int32, (128, 1), 0)

    def contribution(f, source, first):
        chosen = jnp.concatenate([source[first + i] for i in range(8)], axis=1)
        value = chosen[:8] + chosen[8:]
        pixel, cell, used = value[4:5], value[5:6] - first_cell, value[6:7]
        block = jnp.floor(pixel * (1.0 / 128.0))
        low = pixel - 128.0 * block
        pair = jnp.floor(block * 0.25)
        quarter = block - 4.0 * pair
        of_frame = jnp.concatenate([table[pl.ds(pl.multiple_of((2 * i + f) * 48, 48), 48), :] for i in range(32)], axis=0)
        read = jnp.dot(of_frame, where_bf16(low_row == low), preferred_element_type=jnp.float32)
        total = jnp.zeros((48, LANES), jnp.float32)
        for i in range(32):
            total = total + jnp.where(pair == float(i), read[48 * i : 48 * i + 48], 0.0)
        total = jnp.where(quarter_row == quarter, total, 0.0)
        painted = jnp.dot(to_class, total.astype(jnp.bfloat16), preferred_element_type=jnp.float32)
        gate = jax.nn.sigmoid(painted)
        gate_high, gate_low = split(gate)
        features = jnp.concatenate([chosen.astype(jnp.bfloat16), gate_high, gate_low], axis=0)
        both = jnp.dot(wk_both, features, preferred_element_type=jnp.float32)
        hidden = jnp.maximum(both[:64] + both[64:], 0.0)
        row = jnp.floor(cell * (1.0 / 128.0))
        col = cell - 128.0 * row
        row = jnp.where(used > 0.5, row, -1.0)
        by_row = jnp.concatenate(
            [jnp.where(row == float(r), hidden, 0.0) for r in range(3)], axis=0
        ).astype(jnp.bfloat16)
        return lax.dot_general(
            where_bf16(low_row == col), by_row, (((1,), (1,)), ((), ())),
            preferred_element_type=jnp.float32,
        )

    for f in range(2):
        pooled[f] = contribution(f, packed_first, 8 * f)
    for f in range(2):
        most = jnp.max(jnp.maximum(place[2 * f], place[2 * f + 1])) + 1.0
        passes = (most.astype(jnp.int32) + SLOTS - 1) // SLOTS

        def one_pass(number, carry):
            def group(g, state):
                pack_group(points, place, packed, f, g, (number * SLOTS).astype(jnp.float32), g)
                return state

            lax.fori_loop(0, 8, group, 0)
            pooled[f] += contribution(f, packed, 0)
            return carry

        lax.fori_loop(1, passes, one_pass, 0)
    for f in range(2):
        grid = pooled[f]
        total = None
        for d in range(3):
            if d == 0:
                moved = jnp.where(column >= 1, pltpu.roll(grid, 1, 0), 0.0)
            elif d == 2:
                moved = jnp.where(column < 127, pltpu.roll(grid, 127, 0), 0.0)
            else:
                moved = grid
            weight = jnp.concatenate([bev[(3 * r + d) * 64 : (3 * r + d + 1) * 64, :] for r in range(3)], axis=0)
            part = jnp.dot(moved.astype(jnp.bfloat16), weight, preferred_element_type=jnp.float32)
            total = part if total is None else total + part
        feature = jnp.maximum(total, 0.0).astype(jnp.bfloat16)
        out[:, f, :] = lax.dot_general(
            head[...], feature, (((1,), (1,)), ((), ())), preferred_element_type=jnp.float32
        )
    for f in range(2):
        for half in range(2):
            even, odd = sc[f, 11 * half : 11 * half + 11, :], sc[f, 11 * half + 22 : 11 * half + 33, :]
            scores[:, f, 128 * half : 128 * half + 128] = jnp.where(w % 2 == 0, even, odd)


def point_part(points, table, packed, place, sc, pillar, bev, head):
    vmem = pl.BlockSpec(memory_space=pltpu.VMEM)
    return pl.pallas_call(
        point_kernel,
        name="point_part",
        out_shape=(
            jax.ShapeDtypeStruct((20, 2, 128), jnp.float32),
            jax.ShapeDtypeStruct((11, 2, 256), jnp.float32),
        ),
        in_specs=[vmem] * 8,
        out_specs=(vmem, vmem),
        scratch_shapes=[
            pltpu.VMEM((8, 16, SLOTS), jnp.float32),
            pltpu.VMEM((2, 128, 192), jnp.float32),
            pltpu.VMEM((128, 128), jnp.float32),
        ],
        compiler_params=pltpu.CompilerParams(vmem_limit_bytes=40 * 2**20),
        cost_estimate=pl.CostEstimate(flops=10**9, bytes_accessed=3 * 10**6, transcendentals=10**5),
    )(points, table, packed, place, sc, pillar, bev, head)


def local(
    image,
    conv_weight,
    class_weight,
    point_feats,
    pixel_index,
    pillar_index,
    point_counts,
    pillar_weight,
    bev_weight,
    head_weight,
):
    sc, table, points, packed, place = image_part(
        image, conv_weight, class_weight, point_feats, pixel_index, pillar_index, point_counts
    )
    detections, scores = point_part(points, table, packed, place, sc, pillar_weight.T, bev_weight, head_weight.T)
    return (detections.transpose(1, 2, 0), scores.transpose(1, 0, 2))


def solution(mesh):
    placed = (
        P(None, None, "wide"),
        P("phase", None, None),
        P(),
        P("phase", None, "wide"),
        P("phase", "wide"),
        P("phase", "wide"),
        P("phase", "wide"),
        P(),
        P(),
        P(),
    )
    return jax.shard_map(
        local,
        mesh=mesh,
        in_specs=placed,
        out_specs=(P("phase", "wide", None), P("phase", None, "wide")),
        check_vma=False,
    )
```

```python
import functools

import jax
import jax.numpy as jnp
from jax import lax
from jax.experimental import pallas as pl
from jax.experimental.pallas import tpu as pltpu
from jax.sharding import PartitionSpec as P

C = 256
ROWS = 24
MOST_ROWS = 12
MESH = pl.DeviceIdType.MESH
NEAR = (4, -4, 3, -3, 2, -2, 1, -1)
BATCHES = ((3, 9), (12, 4), (0, 3))
PASSED_ON = (((3, 5), (8, 4)), ((12, 4), None), (None, (0, 3)))


SLOTS = 128
GROUP = 16
LANES = 1024


def iota(shape, dim):
    return lax.broadcasted_iota(jnp.int32, shape, dim).astype(jnp.float32)


def where_bf16(mask):
    return jnp.where(mask, jnp.float32(1.0), jnp.float32(0.0)).astype(jnp.bfloat16)


def split(value):
    high = value.astype(jnp.bfloat16)
    return high, (value - high.astype(jnp.float32)).astype(jnp.bfloat16)


def find_places(points, place, f, first_cell):
    row_i = lax.broadcasted_iota(jnp.int32, (128, 128), 0)
    col_i = lax.broadcasted_iota(jnp.int32, (128, 128), 1)
    up_to = where_bf16(row_i <= col_i)
    row_j = lax.broadcasted_iota(jnp.int32, (64, 64), 0)
    col_j = lax.broadcasted_iota(jnp.int32, (64, 64), 1)
    before = where_bf16((row_j // GROUP == col_j // GROUP) & (col_j < row_j))
    all_ones = jnp.ones((128, 128), jnp.bfloat16)
    for h in range(2):
        cell = points[pl.ds((2 * f + h) * 8 + 5, 64, stride=32), :] - first_cell
        mine = (cell >= 0.0) & (cell < 384.0)
        mine_16 = where_bf16(mine)
        inside = jnp.dot(mine_16, up_to, preferred_element_type=jnp.float32)
        row_sum = jnp.dot(mine_16, all_ones, preferred_element_type=jnp.float32)
        ahead = jnp.dot(before, row_sum.astype(jnp.bfloat16), preferred_element_type=jnp.float32)
        place[2 * f + h] = jnp.where(mine, inside - 1.0 + ahead, -1.0)


def pack_group(points, place, packed, f, g, first_slot, where):
    h, first = g // 4, pl.multiple_of(g % 4 * GROUP, GROUP)
    slot = iota((SLOTS, 128), 0) + first_slot
    places = place[2 * f + h, pl.ds(first, GROUP), :]
    data, picks = [], []
    for i in range(GROUP):
        rows = points[pl.ds(pl.multiple_of((first + i) * 32 + (2 * f + h) * 8, 8), 8), :]
        high, low = split(rows)
        data.append(jnp.concatenate([high.astype(jnp.float32), low.astype(jnp.float32)], axis=0))
        picks.append(where_bf16(slot == places[i : i + 1, :]))
    packed[where] = lax.dot_general(
        jnp.concatenate(data, axis=1).astype(jnp.bfloat16), jnp.concatenate(picks, axis=1),
        (((1,), (1,)), ((), ())), preferred_element_type=jnp.float32,
    )


def layers(act, weights, numbers, top_row):
    for number in numbers:
        now, later = number % 2, (number + 1) % 2
        rows = 22 - 2 * number
        half = rows if rows <= MOST_ROWS else (rows + 1) // 2
        for first in range(0, rows, half):
            count = min(half, rows - first) * 64
            start = (number + 1 + first) * 64
            column = lax.broadcasted_iota(jnp.int32, (count, 1), 0) % 64
            row = lax.broadcasted_iota(jnp.int32, (count, 1), 0) // 64 + (top_row + number + 1 + first)
            lhs = jnp.concatenate([act[now, pl.ds(start + 64 * r, count), :] for r in (-1, 0, 1)], axis=1)

            def part(tap):
                rhs = jnp.concatenate(
                    [weights[number, :, (3 * r + tap) * C : (3 * r + tap + 1) * C] for r in range(3)], axis=1
                )
                return lax.dot_general(lhs, rhs, (((1,), (1,)), ((), ())), preferred_element_type=jnp.float32)

            total = part(1)
            total = total + jnp.where(column >= 1, pltpu.roll(part(0), 1, 0), 0.0)
            total = total + jnp.where(column < 63, pltpu.roll(part(2), count - 1, 0), 0.0)
            new = act[now, pl.ds(start, count), :].astype(jnp.float32) + jnp.maximum(total, 0.0)
            new = jnp.where((row >= 0) & (row < 256), new, 0.0)
            act[later, pl.ds(start, count), :] = new.astype(jnp.bfloat16)


def image_kernel(
    image, w_own, class_weight_h, feats_h, pixel_h, pillar_h, counts_h, sc, table, points, packed, place, weights, act, raw, img,
    class_weight, feats, pixel, pillar, counts, own_sem, raw_sem, in_sem, send_sem, h_sem, y1_sem, y2_sem, x1_sem, x2_sem, d_sem, tz_sem, tx_sem, tf_sem,
    pz_sem, px_sem, pf_sem, s_sem, ag_send,
):
    p = lax.axis_index("phase")
    w = lax.axis_index("wide")
    y, c = p // 2, p % 2
    x, z = w // 16, w % 16
    k, t = w // 2, w % 2
    top_row = 8 * k - 8

    def at(phase, wide):
        return {"phase": phase, "wide": wide}

    def y_dev(step):
        return at(2 * ((y + step + 4) % 4) + c, w)

    def x_dev(step):
        return at(p, 16 * ((x + step + 4) % 4) + z)

    def z_dev(step):
        return at(p, 16 * x + (z + step + 16) % 16)

    partner = at(2 * y + 1 - c, w)
    sibling = at(p, 2 * k + 1 - t)
    halo_peers = [(d, f) for d in (-1, 1) for f in (0, 1)]

    raw_copy = pltpu.make_async_copy(image.at[pl.ds(2 * p, 2)], raw, raw_sem)
    raw_copy.start()
    own_copy = pltpu.make_async_copy(w_own.at[0], weights.at[p], own_sem)
    own_copy.start()
    small = [
        pltpu.make_async_copy(src, dst, in_sem.at[i])
        for i, (src, dst) in enumerate(
            ((feats_h, feats), (pixel_h, pixel), (pillar_h, pillar), (counts_h, counts), (class_weight_h, class_weight))
        )
    ]
    for copy in small:
        copy.start()
    barrier = pltpu.get_barrier_semaphore()
    peers = [y_dev(1), y_dev(-1), partner, sibling]
    peers += [x_dev(1), x_dev(-1)] + [z_dev(d) for d in NEAR]
    peers += [at(p, (2 * (k + d) + f + 64) % 64) for d, f in halo_peers]
    for peer in peers:
        pl.semaphore_signal(barrier, inc=1, device_id=peer, device_id_type=MESH)
    for copy in small:
        copy.wait()
    own_slot = 16 * x + 7
    lane = lax.broadcasted_iota(jnp.int32, (1, 256), 1)
    for f in range(2):
        cell = jnp.where(lane < counts[:, f : f + 1], pillar[f : f + 1, :], -1024).astype(jnp.float32)
        where = pixel[f : f + 1, :].astype(jnp.float32)
        for h in range(2):
            first = 32 * own_slot + (2 * f + h) * 8
            points[pl.ds(first, 4), :] = feats[f, :, 128 * h : 128 * h + 128]
            points[pl.ds(first + 4, 1), :] = where[:, 128 * h : 128 * h + 128]
            points[pl.ds(first + 5, 1), :] = cell[:, 128 * h : 128 * h + 128]
            points[pl.ds(first + 6, 2), :] = jnp.ones((2, 128), jnp.float32)
    raw_copy.wait()
    for f in range(2):
        img[f] = jnp.swapaxes(raw[f], 0, 1)
    pl.semaphore_wait(barrier, len(peers))

    sends = []

    def send(src, dst, recv, device):
        number = len(sends)
        copy = pltpu.make_async_remote_copy(
            src_ref=src, dst_ref=dst, send_sem=send_sem.at[number], recv_sem=recv,
            device_id=device, device_id_type=MESH,
        )
        copy.start()
        sends.append(copy)

    def arrived(ref, recv):
        pltpu.make_async_remote_copy(
            src_ref=ref, dst_ref=ref, send_sem=send_sem.at[0], recv_sem=recv,
            device_id=partner, device_id_type=MESH,
        ).wait_recv()

    def block(j):
        return act.at[0, pl.ds(pl.multiple_of(j * 256, 256), 256), :]

    send(img.at[1 - t], block(2 + t), h_sem.at[2 + t], sibling)
    for d, f in halo_peers:
        send(img.at[f], block(2 - 2 * d + t), h_sem.at[2 - 2 * d + t], at(p, (2 * (k + d) + f + 64) % 64))

    def post(src, dst, sem, number, device):
        pltpu.make_async_remote_copy(
            src_ref=src, dst_ref=dst, send_sem=ag_send.at[number], recv_sem=sem,
            device_id=device, device_id_type=MESH,
        ).start()

    class Spread:
        def __init__(self, ref, rows, z_sem, x_sem, f_sem, number):
            self.ref, self.rows, self.number = ref, rows, number
            self.z_sem, self.x_sem, self.f_sem = z_sem, x_sem, f_sem

        def some(self, slot, count, column=0):
            first = 16 * ((x + column + 4) % 4) + slot
            return self.ref.at[pl.ds(pl.multiple_of(self.rows * first, self.rows), self.rows * count)]

        def block(self, d):
            return self.some(d + 7, 1)

        def z_first(self):
            for d in NEAR:
                post(self.block(0), self.block(d), self.z_sem.at[d + 7], self.number, z_dev(d))

        def z_wait(self, *distances):
            for d in distances:
                arrived(self.block(d), self.z_sem.at[d + 7])

        def z_second(self):
            for d in (4, -4):
                self.z_wait(d)
                for e in (4, 3, 2, 1) if d > 0 else (-3, -2, -1):
                    post(self.block(d), self.block(d + e), self.z_sem.at[d + e + 7], self.number, z_dev(e))

        def x_first(self, batch):
            ref = self.some(*BATCHES[batch])
            for side in range(2):
                post(ref, ref, self.x_sem.at[side, batch], self.number, x_dev(1 - 2 * side))

        def x_second(self, batch):
            for side in range(2):
                step = 1 - 2 * side
                arrived(self.some(*BATCHES[batch], -step), self.x_sem.at[side, batch])
                if PASSED_ON[batch][side]:
                    ref = self.some(*PASSED_ON[batch][side], -step)
                    post(ref, ref, self.f_sem, self.number, x_dev(step))

        def last(self):
            arrived(self.some(0, 16, 2), self.f_sem)

        def sent(self):
            ref = self.ref.at[pl.ds(0, 63 * self.rows)]
            pltpu.make_async_remote_copy(
                src_ref=ref, dst_ref=ref, send_sem=ag_send.at[self.number], recv_sem=own_sem,
                device_id=partner, device_id_type=MESH,
            ).wait_send()

    spread_points = Spread(points, 32, pz_sem, px_sem, pf_sem, 0)
    spread_table = Spread(table, 48, tz_sem, tx_sem, tf_sem, 1)

    def q_cols(layer, owner, first=0, tiles=3):
        return weights.at[layer, :, pl.ds(pl.multiple_of(768 + 384 * owner + 128 * first, 128), 128 * tiles)]

    def a_cols(layer, half):
        return weights.at[layer, :, pl.ds(384 * half, 384)]

    def layer_of(step):
        return 2 * ((y + step + 8) % 4) + c

    q_parts = ((0, 2), (2, 1))
    sign = 1 - 2 * c
    steps = (sign, -sign)
    near = [layer_of(-sign), layer_of(sign)]
    far = layer_of(2)
    soon_step = 1 - 2 * (((y + 1) // 2) % 2)
    soon = (1 + soon_step * sign) // 2
    late = 1 - soon
    soon_layer, late_layer = layer_of(soon_step), layer_of(-soon_step)

    def x_first(layer, j):
        for d in range(2):
            send(q_cols(layer, x), q_cols(layer, x), x1_sem.at[d, j], x_dev(steps[d]))

    def x_second(layer, j):
        for d in range(2):
            source = (x - steps[d] + 4) % 4
            arrived(q_cols(layer, source), x1_sem.at[d, j])
            part = q_cols(layer, source, *q_parts[d])
            send(part, part, x2_sem.at[d, j], x_dev(steps[d]))

    def x_done(layer, j):
        for d in range(2):
            arrived(q_cols(layer, (x + 2) % 4, *q_parts[d]), x2_sem.at[d, j])

    def hand_over(layer, half):
        part = weights.at[layer, :, pl.ds(768 * half, 768 + 768 * half)]
        send(part, part, d_sem.at[layer // 2, half], partner)

    def taken_over(number):
        @pl.when(c == 1 - number % 2)
        def _():
            for half in range(2):
                arrived(weights.at[number, :, pl.ds(768 * half, 768 + 768 * half)], d_sem.at[number // 2, half])

    own_copy.wait()
    for d in range(2):
        send(q_cols(p, x), q_cols(p, x), y1_sem.at[d, 0], y_dev(steps[d]))
    hand_over(p, 0)
    hand_over(p, 1)
    spread_points.z_first()
    for d in range(2):
        arrived(q_cols(near[d], x), y1_sem.at[d, 0])
        part = q_cols(near[d], x, *q_parts[d])
        send(part, part, y2_sem.at[d, 0], y_dev(steps[d]))
    x_first(soon_layer, soon)
    for d in range(2):
        send(a_cols(p, d), a_cols(p, d), y1_sem.at[d, 1], y_dev(steps[d]))
    for d in range(2):
        arrived(a_cols(near[d], d), y1_sem.at[d, 1])
        send(a_cols(near[d], d), a_cols(near[d], d), y2_sem.at[d, 1], y_dev(steps[d]))
        send(a_cols(p, 1 - d), a_cols(p, 1 - d), y1_sem.at[d, 2], y_dev(steps[d]))
    for d in range(2):
        arrived(q_cols(far, x, *q_parts[d]), y2_sem.at[d, 0])
    x_first(far, 2)
    x_second(soon_layer, soon)
    x_second(far, 2)
    x_first(late_layer, late)
    for d in range(2):
        arrived(a_cols(far, d), y2_sem.at[d, 1])
    hand_over(far, 0)
    spread_points.z_second()
    for d in range(2):
        arrived(a_cols(near[d], 1 - d), y1_sem.at[d, 2])
    hand_over(soon_layer, 0)
    hand_over(late_layer, 0)
    x_done(soon_layer, soon)
    hand_over(soon_layer, 1)
    x_done(far, 2)
    hand_over(far, 1)

    act[0, pl.ds(pl.multiple_of((2 + t) * 256, 256), 256), :] = img[t]
    for j in (0, 1, 4, 5):
        arrived(block(j), h_sem.at[j])
    arrived(block(3 - t), h_sem.at[3 - t])

    @pl.when(k == 0)
    def _():
        act[0, pl.ds(0, 512), :] = jnp.zeros((512, C), jnp.bfloat16)

    @pl.when(k == 31)
    def _():
        act[0, pl.ds(1024, 512), :] = jnp.zeros((512, C), jnp.bfloat16)

    def layer(number):
        taken_over(number)
        layers(act, weights, (number,), top_row)

    layer(0)
    layer(1)
    x_second(late_layer, late)
    spread_points.z_wait(1, -1, 2, -2, 3, -3, 5, 6, 7, 8, -5, -6, -7)
    for batch in range(3):
        spread_points.x_first(batch)
    layer(2)
    x_done(late_layer, late)
    hand_over(late_layer, 1)
    layer(3)
    layer(4)
    for batch in range(3):
        spread_points.x_second(batch)
    layer(5)
    layer(6)
    layer(7)

    row_i = lax.broadcasted_iota(jnp.int32, (48, 11), 0)
    row_j = lax.broadcasted_iota(jnp.int32, (48, 11), 1)
    placed = []
    for q in range(4):
        here = jnp.where(row_i == row_j + 11 * q, 1.0, 0.0).astype(jnp.bfloat16)
        placed.append(
            jnp.dot(here, class_weight[...], preferred_element_type=jnp.float32).astype(jnp.bfloat16)
        )
    total = None
    for q in range(4):
        part = lax.dot_general(
            placed[q], act[0, pl.ds(512 + 128 * q, 128), :], (((1,), (1,)), ((), ())),
            preferred_element_type=jnp.float32,
        )
        total = part if total is None else total + part
    table[pl.ds(pl.multiple_of(48 * own_slot, 48), 48), :] = total.astype(jnp.bfloat16)
    sc[t] = total
    spread_table.z_first()
    send(sc.at[t], sc.at[t], s_sem, sibling)
    spread_points.last()
    first_cell = ((w - 1) * 128).astype(jnp.float32)
    for f in range(2):
        find_places(points, place, f, first_cell)

    def pack(first, last):
        def one(g, state):
            pack_group(points, place, packed, g // 8, g % 8, 0.0, g)
            return state

        lax.fori_loop(first, last, one, 0)

    pack(0, 6)
    spread_table.z_second()
    spread_table.z_wait(1, -1, 2, -2, 3, -3)
    spread_table.x_first(0)
    pack(6, 12)
    spread_table.x_second(0)
    spread_table.z_wait(5, 6, 7, 8)
    spread_table.x_first(1)
    spread_table.z_wait(-5, -6, -7)
    spread_table.x_first(2)
    pack(12, 16)
    spread_table.x_second(1)
    spread_table.x_second(2)
    spread_points.sent()
    spread_table.last()
    spread_table.sent()
    arrived(sc.at[1 - t], s_sem)
    for copy in sends:
        copy.wait_send()


N_SENDS = 48


def image_part(image, conv_weight, class_weight, feats, pixel, pillar, counts):
    vmem = pl.BlockSpec(memory_space=pltpu.VMEM)
    hbm = pl.BlockSpec(memory_space=pltpu.HBM)
    dma = pltpu.SemaphoreType.DMA
    operands = (image, conv_weight, class_weight, feats, pixel, pillar, counts.reshape(1, 2))
    operands = [pltpu.with_memory_space_constraint(o, pltpu.HBM) for o in operands]
    return pl.pallas_call(
        image_kernel,
        name="image_part",
        out_shape=(
            jax.ShapeDtypeStruct((2, 48, 128), jnp.float32),
            jax.ShapeDtypeStruct((64 * 48, 128), jnp.bfloat16),
            jax.ShapeDtypeStruct((64 * 32, 128), jnp.float32),
            jax.ShapeDtypeStruct((16, 16, SLOTS), jnp.float32),
            jax.ShapeDtypeStruct((4, 64, 128), jnp.float32),
        ),
        in_specs=[hbm] * 7,
        out_specs=(vmem,) * 5,
        scratch_shapes=[
            pltpu.VMEM((8, C, 9 * C), jnp.bfloat16),
            pltpu.VMEM((2, ROWS * 64, C), jnp.bfloat16),
            pltpu.VMEM((2, C, 256), jnp.bfloat16),
            pltpu.VMEM((2, 256, C), jnp.bfloat16),
            pltpu.VMEM((11, C), jnp.bfloat16),
            pltpu.VMEM((2, 4, 256), jnp.float32),
            pltpu.VMEM((2, 256), jnp.int32),
            pltpu.VMEM((2, 256), jnp.int32),
            pltpu.VMEM((1, 2), jnp.int32),
            dma, dma, dma((5,)), dma((N_SENDS,)), dma((6,)), dma((2, 3)), dma((2, 2)), dma((2, 3)), dma((2, 3)), dma((4, 2)),
            dma((16,)), dma((2, 3)), dma, dma((16,)), dma((2, 3)), dma, dma, dma((2,)),
        ],
        compiler_params=pltpu.CompilerParams(
            collective_id=0, has_side_effects=True, vmem_limit_bytes=40 * 2**20
        ),
        cost_estimate=pl.CostEstimate(flops=10**10, bytes_accessed=10**7, transcendentals=0),
    )(*operands)


def point_kernel(points, table, packed_first, place, sc, pillar, bev, head, out, scores, packed, pooled, spare):
    w = lax.axis_index("wide")
    z = w % 16
    first_cell = ((w - 1) * 128).astype(jnp.float32)
    low_row = iota((128, LANES), 0)
    quarter_row = lax.broadcasted_iota(jnp.int32, (48, LANES), 0) // 11
    quarter_row = quarter_row.astype(jnp.float32)
    class_i = lax.broadcasted_iota(jnp.int32, (16, 48), 0)
    class_j = lax.broadcasted_iota(jnp.int32, (16, 48), 1)
    to_class = where_bf16((class_j % 11 == class_i) & (class_j < 44))
    spare[...] = jnp.zeros_like(spare)
    for first in (0, 8):
        spare[first : first + 4, :64] = pillar[:4, :]
    for first in (16, 32):
        spare[first : first + 11, :64] = pillar[4:, :]
    wk_high, wk_low = split(jnp.swapaxes(spare[...], 0, 1)[:64, :48])
    wk_both = jnp.concatenate([wk_high, wk_low], axis=0)
    column = lax.broadcasted_iota(jnp.int32, (128, 1), 0)

    def contribution(f, source, first):
        chosen = jnp.concatenate([source[first + i] for i in range(8)], axis=1)
        value = chosen[:8] + chosen[8:]
        pixel, cell, used = value[4:5], value[5:6] - first_cell, value[6:7]
        block = jnp.floor(pixel * (1.0 / 128.0))
        low = pixel - 128.0 * block
        pair = jnp.floor(block * 0.25)
        quarter = block - 4.0 * pair
        odd = (z + 1 + f) % 2
        rows = [pl.multiple_of(48 * (16 * i + 2 * j + odd), 48) for i in range(4) for j in range(8)]
        of_frame = jnp.concatenate([table[pl.ds(first_row, 48), :] for first_row in rows], axis=0)
        pairs = [8 * i + (z + 23 - 2 * j - odd) % 16 // 2 for i in range(4) for j in range(8)]
        read = jnp.dot(of_frame, where_bf16(low_row == low), preferred_element_type=jnp.float32)
        total = jnp.zeros((48, LANES), jnp.float32)
        for i in range(32):
            total = total + jnp.where(pair == pairs[i].astype(jnp.float32), read[48 * i : 48 * i + 48], 0.0)
        total = jnp.where(quarter_row == quarter, total, 0.0)
        painted = jnp.dot(to_class, total.astype(jnp.bfloat16), preferred_element_type=jnp.float32)
        gate = jax.nn.sigmoid(painted)
        gate_high, gate_low = split(gate)
        features = jnp.concatenate([chosen.astype(jnp.bfloat16), gate_high, gate_low], axis=0)
        both = jnp.dot(wk_both, features, preferred_element_type=jnp.float32)
        hidden = jnp.maximum(both[:64] + both[64:], 0.0)
        row = jnp.floor(cell * (1.0 / 128.0))
        col = cell - 128.0 * row
        row = jnp.where(used > 0.5, row, -1.0)
        by_row = jnp.concatenate(
            [jnp.where(row == float(r), hidden, 0.0) for r in range(3)], axis=0
        ).astype(jnp.bfloat16)
        return lax.dot_general(
            where_bf16(low_row == col), by_row, (((1,), (1,)), ((), ())),
            preferred_element_type=jnp.float32,
        )

    for f in range(2):
        pooled[f] = contribution(f, packed_first, 8 * f)
    for f in range(2):
        most = jnp.max(jnp.maximum(place[2 * f], place[2 * f + 1])) + 1.0
        passes = (most.astype(jnp.int32) + SLOTS - 1) // SLOTS

        def one_pass(number, carry):
            def group(g, state):
                pack_group(points, place, packed, f, g, (number * SLOTS).astype(jnp.float32), g)
                return state

            lax.fori_loop(0, 8, group, 0)
            pooled[f] += contribution(f, packed, 0)
            return carry

        lax.fori_loop(1, passes, one_pass, 0)
    for f in range(2):
        grid = pooled[f]
        total = None
        for d in range(3):
            if d == 0:
                moved = jnp.where(column >= 1, pltpu.roll(grid, 1, 0), 0.0)
            elif d == 2:
                moved = jnp.where(column < 127, pltpu.roll(grid, 127, 0), 0.0)
            else:
                moved = grid
            weight = jnp.concatenate([bev[(3 * r + d) * 64 : (3 * r + d + 1) * 64, :] for r in range(3)], axis=0)
            part = jnp.dot(moved.astype(jnp.bfloat16), weight, preferred_element_type=jnp.float32)
            total = part if total is None else total + part
        feature = jnp.maximum(total, 0.0).astype(jnp.bfloat16)
        out[:, f, :] = lax.dot_general(
            head[...], feature, (((1,), (1,)), ((), ())), preferred_element_type=jnp.float32
        )
    for f in range(2):
        for half in range(2):
            even, odd = sc[f, 11 * half : 11 * half + 11, :], sc[f, 11 * half + 22 : 11 * half + 33, :]
            scores[:, f, 128 * half : 128 * half + 128] = jnp.where(w % 2 == 0, even, odd)


def point_part(points, table, packed, place, sc, pillar, bev, head):
    vmem = pl.BlockSpec(memory_space=pltpu.VMEM)
    return pl.pallas_call(
        point_kernel,
        name="point_part",
        out_shape=(
            jax.ShapeDtypeStruct((20, 2, 128), jnp.float32),
            jax.ShapeDtypeStruct((11, 2, 256), jnp.float32),
        ),
        in_specs=[vmem] * 8,
        out_specs=(vmem, vmem),
        scratch_shapes=[
            pltpu.VMEM((8, 16, SLOTS), jnp.float32),
            pltpu.VMEM((2, 128, 192), jnp.float32),
            pltpu.VMEM((128, 128), jnp.float32),
        ],
        compiler_params=pltpu.CompilerParams(vmem_limit_bytes=40 * 2**20),
        cost_estimate=pl.CostEstimate(flops=10**9, bytes_accessed=3 * 10**6, transcendentals=10**5),
    )(points, table, packed, place, sc, pillar, bev, head)


def local(
    image,
    conv_weight,
    class_weight,
    point_feats,
    pixel_index,
    pillar_index,
    point_counts,
    pillar_weight,
    bev_weight,
    head_weight,
):
    sc, table, points, packed, place = image_part(
        image, conv_weight, class_weight, point_feats, pixel_index, pillar_index, point_counts
    )
    detections, scores = point_part(points, table, packed, place, sc, pillar_weight.T, bev_weight, head_weight.T)
    return (detections.transpose(1, 2, 0), scores.transpose(1, 0, 2))


def solution(mesh):
    placed = (
        P(None, None, "wide"),
        P("phase", None, None),
        P(),
        P("phase", None, "wide"),
        P("phase", "wide"),
        P("phase", "wide"),
        P("phase", "wide"),
        P(),
        P(),
        P(),
    )
    return jax.shard_map(
        local,
        mesh=mesh,
        in_specs=placed,
        out_specs=(P("phase", "wide", None), P("phase", None, "wide")),
        check_vma=False,
    )
```

```python
import functools

import jax
import jax.numpy as jnp
from jax import lax
from jax.experimental import pallas as pl
from jax.experimental.pallas import tpu as pltpu
from jax.sharding import PartitionSpec as P

C = 256
ROWS = 24
MOST_ROWS = 12
MESH = pl.DeviceIdType.MESH
NEAR = (4, -4, 3, -3, 2, -2, 1, -1)
BATCHES = ((3, 9), (12, 4), (0, 3))
PASSED_ON = (((3, 5), (8, 4)), ((12, 4), None), (None, (0, 3)))


SLOTS = 128
GROUP = 16
LANES = 1024


def iota(shape, dim):
    return lax.broadcasted_iota(jnp.int32, shape, dim).astype(jnp.float32)


def where_bf16(mask):
    return jnp.where(mask, jnp.float32(1.0), jnp.float32(0.0)).astype(jnp.bfloat16)


def split(value):
    high = value.astype(jnp.bfloat16)
    return high, (value - high.astype(jnp.float32)).astype(jnp.bfloat16)


def find_places(points, place, f, first_cell):
    row_i = lax.broadcasted_iota(jnp.int32, (128, 128), 0)
    col_i = lax.broadcasted_iota(jnp.int32, (128, 128), 1)
    up_to = where_bf16(row_i <= col_i)
    row_j = lax.broadcasted_iota(jnp.int32, (64, 64), 0)
    col_j = lax.broadcasted_iota(jnp.int32, (64, 64), 1)
    before = where_bf16((row_j // GROUP == col_j // GROUP) & (col_j < row_j))
    all_ones = jnp.ones((128, 128), jnp.bfloat16)
    for h in range(2):
        cell = points[pl.ds((2 * f + h) * 8 + 5, 64, stride=32), :] - first_cell
        mine = (cell >= 0.0) & (cell < 384.0)
        mine_16 = where_bf16(mine)
        inside = jnp.dot(mine_16, up_to, preferred_element_type=jnp.float32)
        row_sum = jnp.dot(mine_16, all_ones, preferred_element_type=jnp.float32)
        ahead = jnp.dot(before, row_sum.astype(jnp.bfloat16), preferred_element_type=jnp.float32)
        place[2 * f + h] = jnp.where(mine, inside - 1.0 + ahead, -1.0)


def pack_group(points, place, packed, f, g, first_slot, where):
    h, first = g // 4, pl.multiple_of(g % 4 * GROUP, GROUP)
    slot = iota((SLOTS, 128), 0) + first_slot
    places = place[2 * f + h, pl.ds(first, GROUP), :]
    data, picks = [], []
    for i in range(GROUP):
        rows = points[pl.ds(pl.multiple_of((first + i) * 32 + (2 * f + h) * 8, 8), 8), :]
        high, low = split(rows)
        data.append(jnp.concatenate([high.astype(jnp.float32), low.astype(jnp.float32)], axis=0))
        picks.append(where_bf16(slot == places[i : i + 1, :]))
    packed[where] = lax.dot_general(
        jnp.concatenate(data, axis=1).astype(jnp.bfloat16), jnp.concatenate(picks, axis=1),
        (((1,), (1,)), ((), ())), preferred_element_type=jnp.float32,
    )


def layers(act, weights, numbers, top_row):
    for number in numbers:
        now, later = number % 2, (number + 1) % 2
        rows = 22 - 2 * number
        half = rows if rows <= MOST_ROWS else (rows + 1) // 2
        for first in range(0, rows, half):
            count = min(half, rows - first) * 64
            start = (number + 1 + first) * 64
            column = lax.broadcasted_iota(jnp.int32, (count, 1), 0) % 64
            row = lax.broadcasted_iota(jnp.int32, (count, 1), 0) // 64 + (top_row + number + 1 + first)
            lhs = jnp.concatenate([act[now, pl.ds(start + 64 * r, count), :] for r in (-1, 0, 1)], axis=1)

            def part(tap):
                rhs = jnp.concatenate(
                    [weights[number, :, (3 * r + tap) * C : (3 * r + tap + 1) * C] for r in range(3)], axis=1
                )
                return lax.dot_general(lhs, rhs, (((1,), (1,)), ((), ())), preferred_element_type=jnp.float32)

            total = part(1)
            total = total + jnp.where(column >= 1, pltpu.roll(part(0), 1, 0), 0.0)
            total = total + jnp.where(column < 63, pltpu.roll(part(2), count - 1, 0), 0.0)
            new = act[now, pl.ds(start, count), :].astype(jnp.float32) + jnp.maximum(total, 0.0)
            new = jnp.where((row >= 0) & (row < 256), new, 0.0)
            act[later, pl.ds(start, count), :] = new.astype(jnp.bfloat16)


def image_kernel(
    image, w_own, class_weight_h, feats_h, pixel_h, pillar_h, counts_h, sc, table, points, packed, place, weights, act, raw, img,
    class_weight, feats, pixel, pillar, counts, own_sem, raw_sem, in_sem, send_sem, h_sem, y1_sem, y2_sem, x1_sem, x2_sem, d_sem, tz_sem, tx_sem, tf_sem,
    pz_sem, px_sem, pf_sem, s_sem, ag_send,
):
    p = lax.axis_index("phase")
    w = lax.axis_index("wide")
    y, c = p // 2, p % 2
    x, z = w // 16, w % 16
    k, t = w // 2, w % 2
    top_row = 8 * k - 8

    def at(phase, wide):
        return {"phase": phase, "wide": wide}

    def y_dev(step):
        return at(2 * ((y + step + 4) % 4) + c, w)

    def x_dev(step):
        return at(p, 16 * ((x + step + 4) % 4) + z)

    def z_dev(step):
        return at(p, 16 * x + (z + step + 16) % 16)

    partner = at(2 * y + 1 - c, w)
    sibling = at(p, 2 * k + 1 - t)
    halo_peers = [(d, f) for d in (-1, 1) for f in (0, 1)]

    raw_copy = pltpu.make_async_copy(image.at[pl.ds(2 * p, 2)], raw, raw_sem)
    raw_copy.start()
    own_copy = pltpu.make_async_copy(w_own.at[0], weights.at[p], own_sem)
    own_copy.start()
    small = [
        pltpu.make_async_copy(src, dst, in_sem.at[i])
        for i, (src, dst) in enumerate(
            ((feats_h, feats), (pixel_h, pixel), (pillar_h, pillar), (counts_h, counts), (class_weight_h, class_weight))
        )
    ]
    for copy in small:
        copy.start()
    barrier = pltpu.get_barrier_semaphore()
    peers = [y_dev(1), y_dev(-1), partner, sibling]
    peers += [x_dev(1), x_dev(-1)] + [z_dev(d) for d in NEAR]
    peers += [at(p, (2 * (k + d) + f + 64) % 64) for d, f in halo_peers]
    for peer in peers:
        pl.semaphore_signal(barrier, inc=1, device_id=peer, device_id_type=MESH)
    for copy in small:
        copy.wait()
    own_slot = 16 * x + 7
    lane = lax.broadcasted_iota(jnp.int32, (1, 256), 1)
    for f in range(2):
        cell = jnp.where(lane < counts[:, f : f + 1], pillar[f : f + 1, :], -1024).astype(jnp.float32)
        where = pixel[f : f + 1, :].astype(jnp.float32)
        for h in range(2):
            first = 32 * own_slot + (2 * f + h) * 8
            points[pl.ds(first, 4), :] = feats[f, :, 128 * h : 128 * h + 128]
            points[pl.ds(first + 4, 1), :] = where[:, 128 * h : 128 * h + 128]
            points[pl.ds(first + 5, 1), :] = cell[:, 128 * h : 128 * h + 128]
            points[pl.ds(first + 6, 2), :] = jnp.ones((2, 128), jnp.float32)
    raw_copy.wait()
    for f in range(2):
        img[f] = jnp.swapaxes(raw[f], 0, 1)
    pl.semaphore_wait(barrier, len(peers))

    sends = []

    def send(src, dst, recv, device):
        number = len(sends)
        copy = pltpu.make_async_remote_copy(
            src_ref=src, dst_ref=dst, send_sem=send_sem.at[number], recv_sem=recv,
            device_id=device, device_id_type=MESH,
        )
        copy.start()
        sends.append(copy)

    def arrived(ref, recv):
        pltpu.make_async_remote_copy(
            src_ref=ref, dst_ref=ref, send_sem=send_sem.at[0], recv_sem=recv,
            device_id=partner, device_id_type=MESH,
        ).wait_recv()

    def block(j):
        return act.at[0, pl.ds(pl.multiple_of(j * 256, 256), 256), :]

    send(img.at[1 - t], block(2 + t), h_sem.at[2 + t], sibling)
    for d, f in halo_peers:
        send(img.at[f], block(2 - 2 * d + t), h_sem.at[2 - 2 * d + t], at(p, (2 * (k + d) + f + 64) % 64))

    def post(src, dst, sem, number, device):
        pltpu.make_async_remote_copy(
            src_ref=src, dst_ref=dst, send_sem=ag_send.at[number], recv_sem=sem,
            device_id=device, device_id_type=MESH,
        ).start()

    class Spread:
        def __init__(self, ref, rows, z_sem, x_sem, f_sem, number):
            self.ref, self.rows, self.number = ref, rows, number
            self.z_sem, self.x_sem, self.f_sem = z_sem, x_sem, f_sem

        def some(self, slot, count, column=0):
            first = 16 * ((x + column + 4) % 4) + slot
            return self.ref.at[pl.ds(pl.multiple_of(self.rows * first, self.rows), self.rows * count)]

        def block(self, d):
            return self.some(d + 7, 1)

        def z_first(self):
            for d in NEAR:
                post(self.block(0), self.block(d), self.z_sem.at[d + 7], self.number, z_dev(d))

        def z_wait(self, *distances):
            for d in distances:
                arrived(self.block(d), self.z_sem.at[d + 7])

        def z_second(self):
            for d in (4, -4):
                self.z_wait(d)
                for e in (4, 3, 2, 1) if d > 0 else (-3, -2, -1):
                    post(self.block(d), self.block(d + e), self.z_sem.at[d + e + 7], self.number, z_dev(e))

        def x_first(self, batch):
            ref = self.some(*BATCHES[batch])
            for side in range(2):
                post(ref, ref, self.x_sem.at[side, batch], self.number, x_dev(1 - 2 * side))

        def x_second(self, batch):
            for side in range(2):
                step = 1 - 2 * side
                arrived(self.some(*BATCHES[batch], -step), self.x_sem.at[side, batch])
                if PASSED_ON[batch][side]:
                    ref = self.some(*PASSED_ON[batch][side], -step)
                    post(ref, ref, self.f_sem, self.number, x_dev(step))

        def last(self):
            arrived(self.some(0, 16, 2), self.f_sem)

        def sent(self):
            ref = self.ref.at[pl.ds(0, 63 * self.rows)]
            pltpu.make_async_remote_copy(
                src_ref=ref, dst_ref=ref, send_sem=ag_send.at[self.number], recv_sem=own_sem,
                device_id=partner, device_id_type=MESH,
            ).wait_send()

    spread_points = Spread(points, 32, pz_sem, px_sem, pf_sem, 0)
    spread_table = Spread(table, 48, tz_sem, tx_sem, tf_sem, 1)

    def q_cols(layer, owner, first=0, tiles=3):
        return weights.at[layer, :, pl.ds(pl.multiple_of(768 + 384 * owner + 128 * first, 128), 128 * tiles)]

    def a_cols(layer, half):
        return weights.at[layer, :, pl.ds(384 * half, 384)]

    def layer_of(step):
        return 2 * ((y + step + 8) % 4) + c

    q_parts = ((0, 2), (2, 1))
    sign = 1 - 2 * c
    steps = (sign, -sign)
    near = [layer_of(-sign), layer_of(sign)]
    far = layer_of(2)
    soon_step = 1 - 2 * (((y + 1) // 2) % 2)
    soon = (1 + soon_step * sign) // 2
    late = 1 - soon
    soon_layer, late_layer = layer_of(soon_step), layer_of(-soon_step)

    def hand_over(layer):
        part = weights.at[layer, :, pl.ds(0, 768)]
        send(part, part, d_sem.at[layer // 2, 4], partner)

    def hand_quarter(layer, owner):
        send(q_cols(layer, owner), q_cols(layer, owner), d_sem.at[layer // 2, owner], partner)

    def taken_over(number):
        @pl.when(c == 1 - number % 2)
        def _():
            arrived(weights.at[number, :, pl.ds(0, 768)], d_sem.at[number // 2, 4])
            for owner in range(4):
                arrived(q_cols(number, owner), d_sem.at[number // 2, owner])

    def x_first(layer, j):
        for d in range(2):
            send(q_cols(layer, x), q_cols(layer, x), x1_sem.at[d, j], x_dev(steps[d]))
        hand_quarter(layer, x)

    def x_second(layer, j):
        for d in range(2):
            source = (x - steps[d] + 4) % 4
            arrived(q_cols(layer, source), x1_sem.at[d, j])
            part = q_cols(layer, source, *q_parts[d])
            send(part, part, x2_sem.at[d, j], x_dev(steps[d]))
            hand_quarter(layer, source)

    def x_done(layer, j):
        for d in range(2):
            arrived(q_cols(layer, (x + 2) % 4, *q_parts[d]), x2_sem.at[d, j])
        hand_quarter(layer, (x + 2) % 4)

    own_copy.wait()
    for d in range(2):
        send(q_cols(p, x), q_cols(p, x), y1_sem.at[d, 0], y_dev(steps[d]))
    hand_over(p)
    for owner in range(4):
        hand_quarter(p, owner)
    spread_points.z_first()
    for d in range(2):
        arrived(q_cols(near[d], x), y1_sem.at[d, 0])
        part = q_cols(near[d], x, *q_parts[d])
        send(part, part, y2_sem.at[d, 0], y_dev(steps[d]))
    x_first(soon_layer, soon)
    for d in range(2):
        send(a_cols(p, d), a_cols(p, d), y1_sem.at[d, 1], y_dev(steps[d]))
    for d in range(2):
        arrived(a_cols(near[d], d), y1_sem.at[d, 1])
        send(a_cols(near[d], d), a_cols(near[d], d), y2_sem.at[d, 1], y_dev(steps[d]))
        send(a_cols(p, 1 - d), a_cols(p, 1 - d), y1_sem.at[d, 2], y_dev(steps[d]))
    for d in range(2):
        arrived(q_cols(far, x, *q_parts[d]), y2_sem.at[d, 0])
    x_first(far, 2)
    x_second(soon_layer, soon)
    x_second(far, 2)
    x_first(late_layer, late)
    for d in range(2):
        arrived(a_cols(far, d), y2_sem.at[d, 1])
    hand_over(far)
    spread_points.z_second()
    for d in range(2):
        arrived(a_cols(near[d], 1 - d), y1_sem.at[d, 2])
    hand_over(soon_layer)
    hand_over(late_layer)
    x_done(soon_layer, soon)
    x_done(far, 2)

    act[0, pl.ds(pl.multiple_of((2 + t) * 256, 256), 256), :] = img[t]
    for j in (0, 1, 4, 5):
        arrived(block(j), h_sem.at[j])
    arrived(block(3 - t), h_sem.at[3 - t])

    @pl.when(k == 0)
    def _():
        act[0, pl.ds(0, 512), :] = jnp.zeros((512, C), jnp.bfloat16)

    @pl.when(k == 31)
    def _():
        act[0, pl.ds(1024, 512), :] = jnp.zeros((512, C), jnp.bfloat16)

    def layer(number):
        taken_over(number)
        layers(act, weights, (number,), top_row)

    layer(0)
    layer(1)
    x_second(late_layer, late)
    spread_points.z_wait(1, -1, 2, -2, 3, -3, 5, 6, 7, 8, -5, -6, -7)
    for batch in range(3):
        spread_points.x_first(batch)
    layer(2)
    x_done(late_layer, late)
    layer(3)
    layer(4)
    for batch in range(3):
        spread_points.x_second(batch)
    layer(5)
    layer(6)
    layer(7)

    row_i = lax.broadcasted_iota(jnp.int32, (48, 11), 0)
    row_j = lax.broadcasted_iota(jnp.int32, (48, 11), 1)
    placed = []
    for q in range(4):
        here = jnp.where(row_i == row_j + 11 * q, 1.0, 0.0).astype(jnp.bfloat16)
        placed.append(
            jnp.dot(here, class_weight[...], preferred_element_type=jnp.float32).astype(jnp.bfloat16)
        )
    total = None
    for q in range(4):
        part = lax.dot_general(
            placed[q], act[0, pl.ds(512 + 128 * q, 128), :], (((1,), (1,)), ((), ())),
            preferred_element_type=jnp.float32,
        )
        total = part if total is None else total + part
    table[pl.ds(pl.multiple_of(48 * own_slot, 48), 48), :] = total.astype(jnp.bfloat16)
    sc[t] = total
    spread_table.z_first()
    send(sc.at[t], sc.at[t], s_sem, sibling)
    spread_points.last()
    first_cell = ((w - 1) * 128).astype(jnp.float32)
    for f in range(2):
        find_places(points, place, f, first_cell)

    def pack(first, last):
        def one(g, state):
            pack_group(points, place, packed, g // 8, g % 8, 0.0, g)
            return state

        lax.fori_loop(first, last, one, 0)

    pack(0, 6)
    spread_table.z_second()
    spread_table.z_wait(1, -1, 2, -2, 3, -3)
    spread_table.x_first(0)
    pack(6, 12)
    spread_table.x_second(0)
    spread_table.z_wait(5, 6, 7, 8)
    spread_table.x_first(1)
    spread_table.z_wait(-5, -6, -7)
    spread_table.x_first(2)
    pack(12, 16)
    spread_table.x_second(1)
    spread_table.x_second(2)
    spread_points.sent()
    spread_table.last()
    spread_table.sent()
    arrived(sc.at[1 - t], s_sem)
    for copy in sends:
        copy.wait_send()


N_SENDS = 52


def image_part(image, conv_weight, class_weight, feats, pixel, pillar, counts):
    vmem = pl.BlockSpec(memory_space=pltpu.VMEM)
    hbm = pl.BlockSpec(memory_space=pltpu.HBM)
    dma = pltpu.SemaphoreType.DMA
    operands = (image, conv_weight, class_weight, feats, pixel, pillar, counts.reshape(1, 2))
    operands = [pltpu.with_memory_space_constraint(o, pltpu.HBM) for o in operands]
    return pl.pallas_call(
        image_kernel,
        name="image_part",
        out_shape=(
            jax.ShapeDtypeStruct((2, 48, 128), jnp.float32),
            jax.ShapeDtypeStruct((64 * 48, 128), jnp.bfloat16),
            jax.ShapeDtypeStruct((64 * 32, 128), jnp.float32),
            jax.ShapeDtypeStruct((16, 16, SLOTS), jnp.float32),
            jax.ShapeDtypeStruct((4, 64, 128), jnp.float32),
        ),
        in_specs=[hbm] * 7,
        out_specs=(vmem,) * 5,
        scratch_shapes=[
            pltpu.VMEM((8, C, 9 * C), jnp.bfloat16),
            pltpu.VMEM((2, ROWS * 64, C), jnp.bfloat16),
            pltpu.VMEM((2, C, 256), jnp.bfloat16),
            pltpu.VMEM((2, 256, C), jnp.bfloat16),
            pltpu.VMEM((11, C), jnp.bfloat16),
            pltpu.VMEM((2, 4, 256), jnp.float32),
            pltpu.VMEM((2, 256), jnp.int32),
            pltpu.VMEM((2, 256), jnp.int32),
            pltpu.VMEM((1, 2), jnp.int32),
            dma, dma, dma((5,)), dma((N_SENDS,)), dma((6,)), dma((2, 3)), dma((2, 2)), dma((2, 3)), dma((2, 3)), dma((4, 5)),
            dma((16,)), dma((2, 3)), dma, dma((16,)), dma((2, 3)), dma, dma, dma((2,)),
        ],
        compiler_params=pltpu.CompilerParams(
            collective_id=0, has_side_effects=True, vmem_limit_bytes=40 * 2**20
        ),
        cost_estimate=pl.CostEstimate(flops=10**10, bytes_accessed=10**7, transcendentals=0),
    )(*operands)


def point_kernel(points, table, packed_first, place, sc, pillar, bev, head, out, scores, packed, pooled, spare):
    w = lax.axis_index("wide")
    z = w % 16
    first_cell = ((w - 1) * 128).astype(jnp.float32)
    low_row = iota((128, LANES), 0)
    quarter_row = lax.broadcasted_iota(jnp.int32, (48, LANES), 0) // 11
    quarter_row = quarter_row.astype(jnp.float32)
    class_i = lax.broadcasted_iota(jnp.int32, (16, 48), 0)
    class_j = lax.broadcasted_iota(jnp.int32, (16, 48), 1)
    to_class = where_bf16((class_j % 11 == class_i) & (class_j < 44))
    spare[...] = jnp.zeros_like(spare)
    for first in (0, 8):
        spare[first : first + 4, :64] = pillar[:4, :]
    for first in (16, 32):
        spare[first : first + 11, :64] = pillar[4:, :]
    wk_high, wk_low = split(jnp.swapaxes(spare[...], 0, 1)[:64, :48])
    wk_both = jnp.concatenate([wk_high, wk_low], axis=0)
    column = lax.broadcasted_iota(jnp.int32, (128, 1), 0)

    def contribution(f, source, first):
        chosen = jnp.concatenate([source[first + i] for i in range(8)], axis=1)
        value = chosen[:8] + chosen[8:]
        pixel, cell, used = value[4:5], value[5:6] - first_cell, value[6:7]
        block = jnp.floor(pixel * (1.0 / 128.0))
        low = pixel - 128.0 * block
        pair = jnp.floor(block * 0.25)
        quarter = block - 4.0 * pair
        odd = (z + 1 + f) % 2
        rows = [pl.multiple_of(48 * (16 * i + 2 * j + odd), 48) for i in range(4) for j in range(8)]
        of_frame = jnp.concatenate([table[pl.ds(first_row, 48), :] for first_row in rows], axis=0)
        pairs = [8 * i + (z + 23 - 2 * j - odd) % 16 // 2 for i in range(4) for j in range(8)]
        read = jnp.dot(of_frame, where_bf16(low_row == low), preferred_element_type=jnp.float32)
        total = jnp.zeros((48, LANES), jnp.float32)
        for i in range(32):
            total = total + jnp.where(pair == pairs[i].astype(jnp.float32), read[48 * i : 48 * i + 48], 0.0)
        total = jnp.where(quarter_row == quarter, total, 0.0)
        painted = jnp.dot(to_class, total.astype(jnp.bfloat16), preferred_element_type=jnp.float32)
        gate = jax.nn.sigmoid(painted)
        gate_high, gate_low = split(gate)
        features = jnp.concatenate([chosen.astype(jnp.bfloat16), gate_high, gate_low], axis=0)
        both = jnp.dot(wk_both, features, preferred_element_type=jnp.float32)
        hidden = jnp.maximum(both[:64] + both[64:], 0.0)
        row = jnp.floor(cell * (1.0 / 128.0))
        col = cell - 128.0 * row
        row = jnp.where(used > 0.5, row, -1.0)
        by_row = jnp.concatenate(
            [jnp.where(row == float(r), hidden, 0.0) for r in range(3)], axis=0
        ).astype(jnp.bfloat16)
        return lax.dot_general(
            where_bf16(low_row == col), by_row, (((1,), (1,)), ((), ())),
            preferred_element_type=jnp.float32,
        )

    for f in range(2):
        pooled[f] = contribution(f, packed_first, 8 * f)
    for f in range(2):
        most = jnp.max(jnp.maximum(place[2 * f], place[2 * f + 1])) + 1.0
        passes = (most.astype(jnp.int32) + SLOTS - 1) // SLOTS

        def one_pass(number, carry):
            def group(g, state):
                pack_group(points, place, packed, f, g, (number * SLOTS).astype(jnp.float32), g)
                return state

            lax.fori_loop(0, 8, group, 0)
            pooled[f] += contribution(f, packed, 0)
            return carry

        lax.fori_loop(1, passes, one_pass, 0)
    for f in range(2):
        grid = pooled[f]
        total = None
        for d in range(3):
            if d == 0:
                moved = jnp.where(column >= 1, pltpu.roll(grid, 1, 0), 0.0)
            elif d == 2:
                moved = jnp.where(column < 127, pltpu.roll(grid, 127, 0), 0.0)
            else:
                moved = grid
            weight = jnp.concatenate([bev[(3 * r + d) * 64 : (3 * r + d + 1) * 64, :] for r in range(3)], axis=0)
            part = jnp.dot(moved.astype(jnp.bfloat16), weight, preferred_element_type=jnp.float32)
            total = part if total is None else total + part
        feature = jnp.maximum(total, 0.0).astype(jnp.bfloat16)
        out[:, f, :] = lax.dot_general(
            head[...], feature, (((1,), (1,)), ((), ())), preferred_element_type=jnp.float32
        )
    for f in range(2):
        for half in range(2):
            even, odd = sc[f, 11 * half : 11 * half + 11, :], sc[f, 11 * half + 22 : 11 * half + 33, :]
            scores[:, f, 128 * half : 128 * half + 128] = jnp.where(w % 2 == 0, even, odd)


def point_part(points, table, packed, place, sc, pillar, bev, head):
    vmem = pl.BlockSpec(memory_space=pltpu.VMEM)
    return pl.pallas_call(
        point_kernel,
        name="point_part",
        out_shape=(
            jax.ShapeDtypeStruct((20, 2, 128), jnp.float32),
            jax.ShapeDtypeStruct((11, 2, 256), jnp.float32),
        ),
        in_specs=[vmem] * 8,
        out_specs=(vmem, vmem),
        scratch_shapes=[
            pltpu.VMEM((8, 16, SLOTS), jnp.float32),
            pltpu.VMEM((2, 128, 192), jnp.float32),
            pltpu.VMEM((128, 128), jnp.float32),
        ],
        compiler_params=pltpu.CompilerParams(vmem_limit_bytes=40 * 2**20),
        cost_estimate=pl.CostEstimate(flops=10**9, bytes_accessed=3 * 10**6, transcendentals=10**5),
    )(points, table, packed, place, sc, pillar, bev, head)


def local(
    image,
    conv_weight,
    class_weight,
    point_feats,
    pixel_index,
    pillar_index,
    point_counts,
    pillar_weight,
    bev_weight,
    head_weight,
):
    sc, table, points, packed, place = image_part(
        image, conv_weight, class_weight, point_feats, pixel_index, pillar_index, point_counts
    )
    detections, scores = point_part(points, table, packed, place, sc, pillar_weight.T, bev_weight, head_weight.T)
    return (detections.transpose(1, 2, 0), scores.transpose(1, 0, 2))


def solution(mesh):
    placed = (
        P(None, None, "wide"),
        P("phase", None, None),
        P(),
        P("phase", None, "wide"),
        P("phase", "wide"),
        P("phase", "wide"),
        P("phase", "wide"),
        P(),
        P(),
        P(),
    )
    return jax.shard_map(
        local,
        mesh=mesh,
        in_specs=placed,
        out_specs=(P("phase", "wide", None), P("phase", None, "wide")),
        check_vma=False,
    )
```
